128 devices in a mesh: grp: 16 (over z, y_hi, core), head: 8 (over y_lo, x).
Axes of the slice: x: 4, y: 4 (y_hi: 2, y_lo: 2; y = y_hi * 2 + y_lo), z: 4, core: 2. Of those that a mesh axis runs over, the one named last changes fastest.
Arguments:
- hidden: bfloat16 [128, 5376], P('grp'), may hold values from -6 to 6
- pre_gain: float32 [5376], replicated, may hold values from 0.5 to 1.5
- query_weight: bfloat16 [5376, 4096], P(None, 'head'), may hold values from -0.078125 to 0.078125
- key_weight: bfloat16 [5376, 2048], P(None, 'head'), may hold values from -0.078125 to 0.078125
- value_weight: bfloat16 [5376, 2048], P(None, 'head'), may hold values from -0.078125 to 0.078125
- out_weight: bfloat16 [4096, 5376], P('head'), may hold values from -0.09375 to 0.09375
- query_norm_gain: float32 [128], replicated, may hold values from 0.1 to 1.9
- key_gain: float32 [128], replicated, may hold values from 0.1 to 1.9
- post_gain: float32 [5376], P('head'), may hold values from 0.1 to 1.9
- text_keys: bfloat16 [128, 1024, 2048], P('grp', None, 'head'), may hold values from -360 to 360
- text_values: bfloat16 [128, 1024, 2048], P('grp', None, 'head'), may hold values from -6 to 6
- text_position: int32 [128], P('grp'), may hold values from 1 to 4095
- image_keys: bfloat16 [384, 256, 2048], P('grp', None, 'head'), may hold values from -360 to 360
- image_values: bfloat16 [384, 256, 2048], P('grp', None, 'head'), may hold values from -6 to 6
- image_owner: int32 [128], replicated, may hold values from 0 to 15, as said below
- image_slot: int32 [128], replicated, may hold values from 0 to 23, as said below
- image_count: int32 [128], replicated, may hold values from 128 to 256, as said below
Outputs:
- updated: bfloat16 [128, 5376], P('grp', 'head')
The draws below stay inside these ranges and needn't reach their ends.
Inputs may be any that keep to these rules, and one draw needn't show every extreme that they name: `image_owner`: each group owns at most 24 requests, and some group owns exactly 24. `image_slot`: requests with the same owner have distinct slots. `image_count`: A multiple of 128.
All inputs are finite; a program needn't handle non-finite values.
Results may differ from the reference program's by a relative error of at most 0.0055.
The reference program's roundings to bfloat16 on the way count: a program that leaves them out, or rounds other values in their place, can miss the bound.
Values may be sent and summed in bfloat16 or wider, within the bound.
A program may use at most 192 MiB of HBM per device.

```python
import math
import jax
import jax.numpy as jnp
from jax import lax

D = 5376
QH = 32
KVH = 16
HD = 128
WINDOW = 1024
IMG = 256
IMG_BLOCK = 128
SLOTS = 24
BATCH = 128
SLOTS_ALL = 384
N_GRP = 16


def scaled_keys(key, count, length, width):
    base = jnp.clip(jax.random.normal(key, (count, length, width), jnp.float32), -6.0, 6.0)
    return base.astype(jnp.bfloat16)


def draw_text_keys(key, part):
    return scaled_keys(jax.random.fold_in(key, 3), BATCH, WINDOW, KVH * HD)


def draw_image_keys(key, part):
    return scaled_keys(jax.random.fold_in(key, 5), SLOTS_ALL, IMG, KVH * HD)


def owner_table(key):
    base = jax.random.fold_in(key, 11)
    hottest = jax.random.randint(base, (), 0, N_GRP)
    order = jax.random.permutation(jax.random.fold_in(base, 1), BATCH)
    ranking = jnp.zeros((BATCH,), jnp.int32).at[order].set(jnp.arange(BATCH, dtype=jnp.int32))
    remain = jnp.maximum(ranking - SLOTS, 0)
    others = (hottest + 1 + remain % (N_GRP - 1)) % N_GRP
    owners = jnp.where(ranking < SLOTS, hottest, others).astype(jnp.int32)
    owner_matches = (owners[:, None] == jnp.arange(N_GRP, dtype=jnp.int32)[None, :]).astype(jnp.int32)
    earlier = jnp.cumsum(owner_matches, 0) - owner_matches
    slotted = jnp.sum(earlier * owner_matches, 1).astype(jnp.int32)
    return (owners, slotted)


def draw_image_owner(key, part):
    return owner_table(key)[0]


def draw_image_slot(key, part):
    return owner_table(key)[1]


def draw_image_count(key, part):
    blocks = jax.random.randint(jax.random.fold_in(key, 13), (BATCH,), 1, IMG // IMG_BLOCK + 1)
    return (blocks * IMG_BLOCK).astype(jnp.int32)


def set_ends(values, rng, low, largest):
    extent = values.shape
    spot = [jax.random.randint(jax.random.fold_in(rng, axis), (), 0, extent[axis]) for axis in range(len(extent))]
    values = values.at[tuple(spot)].set(low)
    longest = extent.index(max(extent))
    spot[longest] = (spot[longest] + 1) % extent[longest]
    return values.at[tuple(spot)].set(largest)


def block_levels(stream_key, shape, pieces, least, top_value):
    def one(dim, shards_of):
        steps = jax.random.uniform(jax.random.fold_in(jax.random.fold_in(stream_key, 6), dim), (shards_of,), jnp.float32, least / len(pieces), top_value / len(pieces))
        return jnp.repeat(jnp.exp(steps), shape[dim] // shards_of).reshape((-1,) + (1,) * (len(shape) - dim - 1))

    level = one(*pieces[0])
    for cut in pieces[1:]:
        level = level * one(*cut)
    return level


def noise(rng, dims, spread, reach, cuts=(), held_as=jnp.bfloat16):
    values = spread * jax.random.normal(rng, dims, jnp.float32)
    if cuts:
        values = values * block_levels(rng, dims, cuts, -0.22, 0.18)
    return jnp.clip(values, -reach, reach).astype(held_as)


def setup_inputs(seed: int = 0) -> dict:
    splits = jax.random.split(jax.random.key(seed), 18)
    hidden = noise(splits[0], (BATCH, D), 1.0, 6.0, ((0, 16),))
    pre_gain = jnp.clip(1.0 + 0.1 * jax.random.normal(splits[1], (D,), jnp.float32), 0.5, 1.5)
    query_weight = noise(splits[2], (D, QH * HD), D ** -0.5, 0.078125, ((1, 8),))
    key_weight = noise(splits[3], (D, KVH * HD), D ** -0.5, 0.078125, ((1, 8),))
    value_weight = noise(splits[4], (D, KVH * HD), D ** -0.5, 0.078125, ((1, 8),))
    out_weight = noise(splits[5], (QH * HD, D), (QH * HD) ** -0.5, 0.09375, ((0, 8),))
    query_norm_gain = jnp.clip(1.0 + 0.18 * jax.random.normal(splits[6], (HD,), jnp.float32), 0.1, 1.9)
    key_gain = jnp.clip(1.0 + 0.18 * jax.random.normal(splits[7], (HD,), jnp.float32), 0.1, 1.9)
    post_gain = jnp.clip(1.0 + 0.18 * jax.random.normal(splits[8], (D,), jnp.float32), 0.1, 1.9)
    text_keys = draw_text_keys(jax.random.fold_in(splits[17], 71), 0)
    text_values = noise(splits[10], (BATCH, WINDOW, KVH * HD), 1.0, 6.0, ((0, 16), (2, 8)))
    text_position = set_ends(jax.random.randint(splits[11], (BATCH,), 1, 4 * WINDOW), jax.random.fold_in(splits[11], 1), 1, (4 * WINDOW) - 1).astype(jnp.int32)
    image_keys = draw_image_keys(jax.random.fold_in(splits[17], 71), 0)
    image_values = noise(splits[13], (SLOTS_ALL, IMG, KVH * HD), 1.0, 6.0, ((0, 16), (2, 8)))
    image_owner = draw_image_owner(jax.random.fold_in(splits[17], 71), 0)
    image_slot = draw_image_slot(jax.random.fold_in(splits[17], 71), 0)
    image_count = draw_image_count(jax.random.fold_in(splits[17], 71), 0)
    return dict(hidden=hidden, pre_gain=pre_gain, query_weight=query_weight, key_weight=key_weight, value_weight=value_weight, out_weight=out_weight, query_norm_gain=query_norm_gain, key_gain=key_gain, post_gain=post_gain, text_keys=text_keys, text_values=text_values, text_position=text_position, image_keys=image_keys, image_values=image_values, image_owner=image_owner, image_slot=image_slot, image_count=image_count)


EPS = 1e-06

def norm_rows(values, gain):
    values = values.astype(jnp.float32)
    mean_sq = lax.optimization_barrier(jnp.mean(values * values, axis=-1, keepdims=True))
    return values * lax.rsqrt(mean_sq + EPS) * gain.astype(jnp.float32)

def rotate(values, position):
    half = values.shape[-1] // 2
    freq = jnp.exp(-jnp.log(1000000.0) * jnp.arange(half, dtype=jnp.float32) / half)
    angle = position.astype(jnp.float32)[:, None] * freq[None, :]
    cosine = jnp.cos(angle)[:, None, :]
    sine = jnp.sin(angle)[:, None, :]
    first = values[..., :half]
    second = values[..., half:]
    return jnp.concatenate([first * cosine - second * sine, second * cosine + first * sine], axis=-1)

def weigh(scores, valid):
    scores = jnp.where(valid, scores, -1e+30)
    top = lax.optimization_barrier(jnp.max(scores, -1))
    weights = jnp.where(valid, jnp.exp(scores - top[..., None]), 0.0).astype(jnp.bfloat16)
    return (top, weights, lax.optimization_barrier(jnp.sum(weights.astype(jnp.float32), -1)))

def request_block(query_vector, keys, values, valid):
    length = keys.shape[0]
    heads, head_dim = (query_vector.shape[0], query_vector.shape[2])
    keys4 = keys.reshape(length, heads, head_dim).astype(jnp.float32)
    values4 = values.reshape(length, heads, head_dim).astype(jnp.float32)
    scores = jnp.einsum('kgd,lkd->kgl', query_vector.astype(jnp.float32), keys4)
    top, weights, total = weigh(scores, valid[None, None, :])
    summed = jnp.einsum('kgl,lkd->kgd', weights.astype(jnp.float32), values4)
    return (top, total, summed)

def combine(parts, own_token_score, self_value):
    top = own_token_score
    for part in parts:
        top = jnp.maximum(top, part[0])
    total = jnp.exp(own_token_score - top)
    summed = self_value.astype(jnp.float32)[:, :, None, :] * total[..., None]
    for part_top, part_total, part_sum in parts:
        factor = jnp.exp(part_top - top)
        total = total + part_total * factor
        summed = summed + part_sum * factor[..., None]
    return summed / total[..., None]

def reference(hidden, pre_gain, query_weight, key_weight, value_weight, out_weight, query_norm_gain, key_gain, post_gain, text_keys, text_values, text_position, image_keys, image_values, image_owner, image_slot, image_count):
    group = QH // KVH
    normed = norm_rows(hidden, pre_gain).astype(jnp.bfloat16)
    query_vector = jnp.dot(normed, query_weight, preferred_element_type=jnp.float32).reshape(BATCH, QH, HD)
    query_vector = rotate(norm_rows(query_vector, query_norm_gain), text_position) * (1.0 / math.sqrt(D // QH))
    query_vector = query_vector.astype(jnp.bfloat16).reshape(BATCH, KVH, group, HD)
    fresh_key = jnp.dot(normed, key_weight, preferred_element_type=jnp.float32).reshape(BATCH, KVH, HD)
    fresh_key = rotate(norm_rows(fresh_key, key_gain), text_position).astype(jnp.bfloat16)
    value_new = jnp.dot(normed, value_weight, preferred_element_type=jnp.float32).astype(jnp.bfloat16).reshape(BATCH, KVH, HD)
    own_token_score = jnp.einsum('fyeh,fyh->fye', query_vector.astype(jnp.float32), fresh_key.astype(jnp.float32))
    places = jnp.arange(WINDOW, dtype=jnp.int32)
    text_valid = (places[None, :] < text_position[:, None]) & (places[None, :] != (text_position % WINDOW)[:, None])
    text_part = lax.map(lambda item: request_block(*item), (query_vector, text_keys, text_values, text_valid))
    stored = (image_owner * SLOTS + image_slot).astype(jnp.int32)
    image_valid = jnp.arange(IMG, dtype=jnp.int32)[None, :] < image_count[:, None]

    def image_request(item):
        single_query, index, valid = item
        return request_block(single_query, image_keys[index], image_values[index], valid)
    image_part = lax.map(image_request, (query_vector, stored, image_valid))
    attended = combine((image_part, text_part), own_token_score, value_new).astype(jnp.bfloat16).reshape(BATCH, QH * HD)
    projected = jnp.dot(attended, out_weight, preferred_element_type=jnp.float32)
    return (hidden.astype(jnp.float32) + norm_rows(projected, post_gain)).astype(jnp.bfloat16)
```

```python
import functools
import math

import jax
import jax.numpy as jnp
from jax import lax
from jax.experimental import pallas as pl
from jax.experimental.pallas import tpu as pltpu
from jax.sharding import PartitionSpec as P

D = 5376
QH = 32
HD = 128
EPS = 1e-06
BASE = 1000000.0
F32 = jnp.float32
BF16 = jnp.bfloat16
NEG = -1e30

GROUPS = 16
HEADS = 8
ROWS = 8
QHEADS = 4
KVW = 256
WINDOW = 1024
IMG = 256
SLOTS = 24
WIDTH = D // HEADS
WIDTH_PAD = 768
Q_CHUNK = 768
KV_CHUNK = 1792
OW_CHUNK = 1792
IMG_STEP = 8
TEXT_STEP = 2


def iota(shape, dim):
    return lax.broadcasted_iota(jnp.int32, shape, dim)


def matmul(a, b):
    return jnp.dot(a, b, preferred_element_type=F32)


def matmul_t(a, b):
    return lax.dot_general(a, b, (((1,), (1,)), ((), ())), preferred_element_type=F32)


def block_diagonal(x):
    row = iota(x.shape, 0) % 8
    left = jnp.where(row < 2, x, 0.0)
    right = jnp.where(row >= 2, x, 0.0)
    return jnp.concatenate([left, right], axis=1).astype(BF16)


def own_half(x):
    row = iota((x.shape[0], HD), 0) % 8
    return jnp.where(row < 2, x[:, :HD], x[:, HD:])


def layer_kernel(
    hidden, pre_gain, qw, kw, vw, ow, q_gain, k_gain, post_gain, tk, tv, pos, ik, iv, owner, slot, count,
    out,
    hid_v, pre_v, qw_v, kw_v, vw_v, ow_v, qg_v, kg_v, post_v, tk_v, tv_v, pos_v, ik_v, iv_v, own_v, slot_v, cnt_v,
    q_rows, q_send, q_recv, s_text, o_text, m_text, l_text, s_img, o_img, back_send, back_recv,
    proj, rs_send, rs_recv, ss_send, ss_recv,
    small_sem, load_sem, q_ssem, q_rsem, b_ssem, b_rsem, r_ssem, r_rsem, s_ssem, s_rsem,
):
    g = lax.axis_index("grp")
    h = lax.axis_index("head")

    small = [
        (hidden, hid_v),
        (pre_gain, pre_v),
        (q_gain, qg_v),
        (k_gain, kg_v),
        (post_gain, post_v),
        (pos, pos_v),
        (owner, own_v),
        (slot, slot_v),
        (count, cnt_v),
    ]
    small_copies = [pltpu.make_async_copy(a, b, small_sem.at[i]) for i, (a, b) in enumerate(small)]
    loads = []

    def load(src, dst):
        copy = pltpu.make_async_copy(src, dst, load_sem.at[len(loads)])
        loads.append(copy)
        return copy

    q_loads = [load(qw.at[pl.ds(c, Q_CHUNK)], qw_v.at[pl.ds(c, Q_CHUNK)]) for c in range(0, D, Q_CHUNK)]
    k_loads = [load(kw.at[pl.ds(c, KV_CHUNK)], kw_v.at[pl.ds(c, KV_CHUNK)]) for c in range(0, D, KV_CHUNK)]
    v_loads = [load(vw.at[pl.ds(c, KV_CHUNK)], vw_v.at[pl.ds(c, KV_CHUNK)]) for c in range(0, D, KV_CHUNK)]
    ik_loads = [load(ik.at[pl.ds(j, IMG_STEP)], ik_v.at[pl.ds(j, IMG_STEP)]) for j in range(0, SLOTS, IMG_STEP)]
    iv_loads = [load(iv.at[pl.ds(j, IMG_STEP)], iv_v.at[pl.ds(j, IMG_STEP)]) for j in range(0, SLOTS, IMG_STEP)]
    tk_loads = [load(tk.at[pl.ds(b, TEXT_STEP)], tk_v.at[pl.ds(b, TEXT_STEP)]) for b in range(0, ROWS, TEXT_STEP)]
    tv_loads = [load(tv.at[pl.ds(b, TEXT_STEP)], tv_v.at[pl.ds(b, TEXT_STEP)]) for b in range(0, ROWS, TEXT_STEP)]
    o_loads = [load(ow.at[:, pl.ds(c, OW_CHUNK)], ow_v.at[:, pl.ds(c, OW_CHUNK)]) for c in range(0, D, OW_CHUNK)]
    for copy in small_copies:
        copy.start()
    for copy in loads:
        copy.start()

    barrier = pltpu.get_barrier_semaphore()
    for k in range(1, GROUPS):
        pl.semaphore_signal(barrier, inc=1, device_id={"grp": (g + k) % GROUPS})
    for k in range(1, HEADS):
        pl.semaphore_signal(barrier, inc=1, device_id={"head": (h + k) % HEADS})

    for copy in small_copies:
        copy.wait()

    x = hid_v[...].astype(F32)
    mean_sq = jnp.mean(x * x, axis=-1, keepdims=True)
    normed = (x * lax.rsqrt(mean_sq + EPS) * pre_v[...]).astype(BF16)

    lane = iota((ROWS, HD), 1)
    pos_col = jnp.sum(
        jnp.where(iota((ROWS, ROWS), 0) == iota((ROWS, ROWS), 1), pos_v[...].astype(F32), 0.0), axis=1, keepdims=True
    )
    freq = jnp.exp(-math.log(BASE) * (lane % 64).astype(F32) / 64.0)
    angle = pos_col * freq
    cosine = jnp.cos(angle)
    sine = jnp.where(lane < 64, -jnp.sin(angle), jnp.sin(angle))

    def head_norm(v, gain):
        ms = jnp.mean(v * v, axis=-1, keepdims=True)
        v = v * lax.rsqrt(ms + EPS) * gain
        return v * cosine + pltpu.roll(v, 64, 1) * sine

    acc = jnp.zeros((ROWS, QHEADS * HD), F32)
    for i, copy in enumerate(q_loads):
        copy.wait()
        c = i * Q_CHUNK
        acc = acc + matmul(normed[:, c : c + Q_CHUNK], qw_v[pl.ds(c, Q_CHUNK), :])
    queries = []
    for i in range(QHEADS):
        q = head_norm(acc[:, i * HD : (i + 1) * HD], qg_v[...]) * (1.0 / math.sqrt(D // QH))
        queries.append(q.astype(BF16).astype(F32))
    for i in range(8):
        q_rows[pl.ds(i * ROWS, ROWS), :] = queries[i] if i < QHEADS else jnp.zeros((ROWS, HD), F32)
    packed = jnp.concatenate(queries, axis=0).astype(BF16)
    q_send[...] = packed
    q_recv[g] = packed

    pl.semaphore_wait(barrier, GROUPS - 1 + HEADS - 1)

    def to_group(k):
        peer = (g + k) % GROUPS
        return pltpu.make_async_remote_copy(
            src_ref=q_send, dst_ref=q_recv.at[g], send_sem=q_ssem.at[k], recv_sem=q_rsem.at[g], device_id={"grp": peer}
        )

    def from_group(k):
        peer = (g + k) % GROUPS
        return pltpu.make_async_remote_copy(
            src_ref=q_send, dst_ref=q_recv.at[peer], send_sem=q_ssem.at[k], recv_sem=q_rsem.at[peer],
            device_id={"grp": peer},
        )

    for k in range(1, GROUPS):
        to_group(k).start()

    k_acc = jnp.zeros((ROWS, KVW), F32)
    v_acc = jnp.zeros((ROWS, KVW), F32)
    for i in range(len(k_loads)):
        c = i * KV_CHUNK
        k_loads[i].wait()
        k_acc = k_acc + matmul(normed[:, c : c + KV_CHUNK], kw_v[pl.ds(c, KV_CHUNK), :])
    for i in range(len(v_loads)):
        c = i * KV_CHUNK
        v_loads[i].wait()
        v_acc = v_acc + matmul(normed[:, c : c + KV_CHUNK], vw_v[pl.ds(c, KV_CHUNK), :])
    new_keys = [head_norm(k_acc[:, i * HD : (i + 1) * HD], kg_v[...]).astype(BF16).astype(F32) for i in range(2)]
    new_values = [v_acc[:, i * HD : (i + 1) * HD].astype(BF16).astype(F32) for i in range(2)]
    self_score = [jnp.sum(queries[i] * new_keys[i // 2], axis=-1, keepdims=True) for i in range(QHEADS)]

    code = (own_v[...] * 32 + slot_v[...]).astype(F32)
    counts = cnt_v[...].astype(F32)
    mine = (g * 32).astype(F32)
    n_req = GROUPS * ROWS
    slot_row = mine + (iota((SLOTS * 8, n_req), 0) // 8).astype(F32)
    hit = slot_row == code
    r_row = iota((SLOTS * 8, n_req), 0) % 8
    pick = jnp.concatenate([jnp.where(hit & (r_row == i), 1.0, 0.0) for i in range(QHEADS)], axis=1).astype(BF16)
    slot_count = jnp.sum(jnp.where(hit, counts, 0.0), axis=1, keepdims=True)
    code_col = jnp.sum(
        jnp.where(iota((n_req, n_req), 0) == iota((n_req, n_req), 1), code, 0.0), axis=1, keepdims=True
    )
    slot_lane = mine + (iota((n_req, 256), 1) // 8).astype(F32)
    hit_back = code_col == slot_lane
    r_lane = iota((n_req, 256), 1) % 8
    in_store = iota((n_req, 256), 1) < SLOTS * 8
    put = jnp.concatenate(
        [jnp.where(hit_back & in_store & (r_lane == i), 1.0, 0.0) for i in range(QHEADS)], axis=0
    ).astype(BF16)

    for k in range(1, GROUPS):
        from_group(k).wait_recv()
    pieces = [q_recv[p].astype(F32) for p in range(GROUPS)]
    every = jnp.concatenate(
        [pieces[p][i * ROWS : (i + 1) * ROWS] for i in range(QHEADS) for p in range(GROUPS)], axis=0
    ).astype(BF16)
    asked = block_diagonal(matmul(pick, every))
    for step in range(SLOTS // IMG_STEP):
        ik_loads[step].wait()
        for j in range(step * IMG_STEP, (step + 1) * IMG_STEP):
            s_img[pl.ds(j * 8, 8), :] = matmul_t(asked[j * 8 : (j + 1) * 8], ik_v[j])
    s = s_img[...]
    valid = iota((SLOTS * 8, IMG), 1).astype(F32) < slot_count
    s = jnp.where(valid, s, NEG)
    top = jnp.max(s, axis=-1, keepdims=True)
    weights = jnp.where(valid, jnp.exp(s - top), 0.0).astype(BF16)
    total = jnp.sum(weights.astype(F32), axis=-1, keepdims=True)
    for step in range(SLOTS // IMG_STEP):
        iv_loads[step].wait()
        for j in range(step * IMG_STEP, (step + 1) * IMG_STEP):
            o_img[pl.ds(j * 8, 8), :] = own_half(matmul(weights[j * 8 : (j + 1) * 8], iv_v[j]))
    some = total > 0.0
    safe = jnp.where(some, total, 1.0)
    mean_value = (o_img[...] / safe).astype(BF16)
    level = jnp.where(some, top + jnp.log(safe), 0.0)
    high = level.astype(BF16).astype(F32)
    middle = (level - high).astype(BF16).astype(F32)
    low = level - high - middle
    part = iota((SLOTS * 8, HD), 1) % 32 // 8
    right_head = iota((SLOTS * 8, HD), 1) // 32 == iota((SLOTS * 8, HD), 0) % 8
    level_parts = jnp.where(part == 0, high, jnp.where(part == 1, middle, jnp.where(part == 2, low, 0.0)))
    level_parts = jnp.where(right_head, level_parts, 0.0).astype(BF16)
    table = jnp.concatenate([mean_value, level_parts], axis=1)
    table = jnp.concatenate([table, jnp.zeros((256 - SLOTS * 8, 256), BF16)], axis=0)
    back = matmul(put, table)
    for p in range(GROUPS):
        rows = [back[i * n_req + p * ROWS : i * n_req + (p + 1) * ROWS] for i in range(QHEADS)]
        levels = rows[0][:, HD:] + rows[1][:, HD:] + rows[2][:, HD:] + rows[3][:, HD:]
        slab = jnp.concatenate([r[:, :HD] for r in rows] + [levels, jnp.zeros((ROWS, HD), F32)], axis=0)
        back_send[p] = slab.astype(BF16)

    def back_to(k):
        peer = (g + k) % GROUPS
        return pltpu.make_async_remote_copy(
            src_ref=back_send.at[peer], dst_ref=back_recv.at[g], send_sem=b_ssem.at[k], recv_sem=b_rsem.at[g],
            device_id={"grp": peer},
        )

    def back_from(k):
        peer = (g + k) % GROUPS
        return pltpu.make_async_remote_copy(
            src_ref=back_send.at[peer], dst_ref=back_recv.at[peer], send_sem=b_ssem.at[k], recv_sem=b_rsem.at[peer],
            device_id={"grp": peer},
        )

    for k in range(1, GROUPS):
        back_to(k).start()
    back_recv[g] = back_send[g]

    for b in range(ROWS):
        if b % TEXT_STEP == 0:
            tk_loads[b // TEXT_STEP].wait()
        q = block_diagonal(q_rows[pl.ds(b, 8, stride=8), :])
        s_text[pl.ds(b * 8, 8), :] = matmul_t(q, tk_v[b])
    place = iota((8, WINDOW), 1)
    for b in range(ROWS):
        if b % TEXT_STEP == 0:
            tv_loads[b // TEXT_STEP].wait()
        p = jnp.sum(jnp.where(iota((8, ROWS), 1) == b, pos_v[...].astype(F32), 0.0), axis=1, keepdims=True)
        p = p.astype(jnp.int32)
        ok = (place < p) & (place != p % WINDOW)
        s = jnp.where(ok, s_text[pl.ds(b * 8, 8), :], NEG)
        top = jnp.max(s, axis=-1, keepdims=True)
        w = jnp.where(ok, jnp.exp(s - top), 0.0).astype(BF16)
        total = jnp.sum(w.astype(F32), axis=-1, keepdims=True)
        o_text[pl.ds(b * 8, 8), :] = own_half(matmul(w, tv_v[b]))
        m_text[pl.ds(b * 8, 8), :] = jnp.broadcast_to(top, (8, HD))
        l_text[pl.ds(b * 8, 8), :] = jnp.broadcast_to(total, (8, HD))

    for k in range(1, GROUPS):
        back_from(k).wait_recv()
    image = back_recv[0].astype(F32)
    for p in range(1, GROUPS):
        image = image + back_recv[p].astype(F32)
    levels = image[QHEADS * ROWS : QHEADS * ROWS + ROWS]
    levels = levels + pltpu.roll(levels, HD - 8, 1) + pltpu.roll(levels, HD - 16, 1)
    attended = []
    for i in range(QHEADS):
        level = jnp.broadcast_to(levels[:, i * 32 : i * 32 + 1], (ROWS, HD))
        mt = m_text[pl.ds(i, ROWS, stride=8), :]
        lt = l_text[pl.ds(i, ROWS, stride=8), :]
        ot = o_text[pl.ds(i, ROWS, stride=8), :]
        own = jnp.broadcast_to(self_score[i], (ROWS, HD))
        top = jnp.maximum(jnp.maximum(level, mt), own)
        from_image = jnp.exp(level - top)
        from_text = jnp.exp(mt - top)
        from_self = jnp.exp(own - top)
        summed = image[i * ROWS : (i + 1) * ROWS] * from_image + ot * from_text + new_values[i // 2] * from_self
        attended.append(summed / (from_image + lt * from_text + from_self))
    attended = jnp.concatenate(attended, axis=1).astype(BF16)

    for i, copy in enumerate(o_loads):
        copy.wait()
        cols = pl.ds(i * OW_CHUNK, OW_CHUNK)
        proj[:, cols] = matmul(attended, ow_v[:, cols])
    for p in range(HEADS):
        start, shift = p * WIDTH // 128 * 128, p * WIDTH % 128
        piece = proj[:, pl.ds(start, WIDTH_PAD)]
        rs_send[p] = pltpu.roll(piece, WIDTH_PAD - shift, 1) if shift else piece

    def share_to(k):
        peer = (h + k) % HEADS
        return pltpu.make_async_remote_copy(
            src_ref=rs_send.at[peer], dst_ref=rs_recv.at[h], send_sem=r_ssem.at[k], recv_sem=r_rsem.at[h],
            device_id={"head": peer},
        )

    def share_from(k):
        peer = (h + k) % HEADS
        return pltpu.make_async_remote_copy(
            src_ref=rs_send.at[peer], dst_ref=rs_recv.at[peer], send_sem=r_ssem.at[k], recv_sem=r_rsem.at[peer],
            device_id={"head": peer},
        )

    for k in range(1, HEADS):
        share_to(k).start()

    start = pl.multiple_of(h * WIDTH // 128 * 128, 128)
    aligned = hid_v[:, pl.ds(start, WIDTH_PAD)].astype(F32)
    residual = aligned
    for c in range(1, 4):
        residual = jnp.where(h % 4 == c, pltpu.roll(aligned, WIDTH_PAD - 32 * c, 1), residual)

    share = rs_send[h]
    for k in range(1, HEADS):
        share_from(k).wait_recv()
        share = share + rs_recv[(h + k) % HEADS]
    share = share[:, :WIDTH]
    squares = jnp.broadcast_to(jnp.sum(share * share, axis=-1, keepdims=True), (ROWS, 128))
    ss_send[...] = squares

    def squares_to(k):
        peer = (h + k) % HEADS
        return pltpu.make_async_remote_copy(
            src_ref=ss_send, dst_ref=ss_recv.at[h], send_sem=s_ssem.at[k], recv_sem=s_rsem.at[h],
            device_id={"head": peer},
        )

    def squares_from(k):
        peer = (h + k) % HEADS
        return pltpu.make_async_remote_copy(
            src_ref=ss_send, dst_ref=ss_recv.at[peer], send_sem=s_ssem.at[k], recv_sem=s_rsem.at[peer],
            device_id={"head": peer},
        )

    for k in range(1, HEADS):
        squares_to(k).start()
    for k in range(1, HEADS):
        squares_from(k).wait_recv()
        squares = squares + ss_recv[(h + k) % HEADS]
    scale = lax.rsqrt(squares[:, :1] / D + EPS)
    out[...] = (residual[:, :WIDTH] + share * scale * post_v[...]).astype(BF16)

    for k in range(1, GROUPS):
        to_group(k).wait_send()
        back_to(k).wait_send()
    for k in range(1, HEADS):
        share_to(k).wait_send()
        squares_to(k).wait_send()


def local(*args):
    (hidden, pre_gain, qw, kw, vw, ow, q_gain, k_gain, post_gain, tk, tv, pos, ik, iv, owner, slot, count) = args
    row = lambda v: v.reshape(1, -1)
    operands = [
        hidden, row(pre_gain), qw, kw, vw, ow, row(q_gain), row(k_gain), row(post_gain), tk, tv, row(pos), ik, iv,
        row(owner), row(slot), row(count),
    ]
    shapes = [pltpu.VMEM(v.shape, v.dtype) for v in operands]
    dma = pltpu.SemaphoreType.DMA
    n_loads = D // Q_CHUNK + 2 * (D // KV_CHUNK) + D // OW_CHUNK + 2 * (SLOTS // IMG_STEP) + 2 * (ROWS // TEXT_STEP)
    scratch = shapes + [
        pltpu.VMEM((64, HD), F32),
        pltpu.VMEM((QHEADS * ROWS, HD), BF16),
        pltpu.VMEM((GROUPS, QHEADS * ROWS, HD), BF16),
        pltpu.VMEM((ROWS * 8, WINDOW), F32),
        pltpu.VMEM((ROWS * 8, HD), F32),
        pltpu.VMEM((ROWS * 8, HD), F32),
        pltpu.VMEM((ROWS * 8, HD), F32),
        pltpu.VMEM((SLOTS * 8, IMG), F32),
        pltpu.VMEM((SLOTS * 8, HD), F32),
        pltpu.VMEM((GROUPS, 48, HD), BF16),
        pltpu.VMEM((GROUPS, 48, HD), BF16),
        pltpu.VMEM((ROWS, D), F32),
        pltpu.VMEM((HEADS, ROWS, WIDTH_PAD), F32),
        pltpu.VMEM((HEADS, ROWS, WIDTH_PAD), F32),
        pltpu.VMEM((ROWS, 128), F32),
        pltpu.VMEM((HEADS, ROWS, 128), F32),
        dma((9,)),
        dma((n_loads,)),
        dma((GROUPS,)),
        dma((GROUPS,)),
        dma((GROUPS,)),
        dma((GROUPS,)),
        dma((HEADS,)),
        dma((HEADS,)),
        dma((HEADS,)),
        dma((HEADS,)),
    ]
    return pl.pallas_call(
        layer_kernel,
        out_shape=jax.ShapeDtypeStruct((ROWS, WIDTH), BF16),
        in_specs=[pl.BlockSpec(memory_space=pl.ANY)] * len(operands),
        out_specs=pl.BlockSpec(memory_space=pltpu.VMEM),
        scratch_shapes=scratch,
        compiler_params=pltpu.CompilerParams(
            collective_id=0, has_side_effects=True, vmem_limit_bytes=60 * 1024 * 1024
        ),
    )(*operands)


def solution(mesh):
    placed = (
        P("grp", None),
        P(),
        P(None, "head"),
        P(None, "head"),
        P(None, "head"),
        P("head", None),
        P(),
        P(),
        P("head"),
        P("grp", None, "head"),
        P("grp", None, "head"),
        P("grp"),
        P("grp", None, "head"),
        P("grp", None, "head"),
        P(),
        P(),
        P(),
    )
    return jax.shard_map(
        local, mesh=mesh, in_specs=placed, out_specs=P("grp", "head"), check_vma=False
    )
```

```python
import functools
import math

import jax
import jax.numpy as jnp
from jax import lax
from jax.experimental import pallas as pl
from jax.experimental.pallas import tpu as pltpu
from jax.sharding import PartitionSpec as P

D = 5376
QH = 32
HD = 128
EPS = 1e-06
BASE = 1000000.0
F32 = jnp.float32
BF16 = jnp.bfloat16
NEG = -1e30

GROUPS = 16
HEADS = 8
ROWS = 8
QHEADS = 4
KVW = 256
WINDOW = 1024
IMG = 256
SLOTS = 24
WIDTH = D // HEADS
WIDTH_PAD = 768
Q_CHUNK = 768
KV_CHUNK = 1792
OW_CHUNK = 1792
IMG_STEP = 8
TEXT_STEP = 2
IN_FLIGHT = 7


def iota(shape, dim):
    return lax.broadcasted_iota(jnp.int32, shape, dim)


def matmul(a, b):
    return jnp.dot(a, b, preferred_element_type=F32)


def matmul_t(a, b):
    return lax.dot_general(a, b, (((1,), (1,)), ((), ())), preferred_element_type=F32)


def block_diagonal(x):
    row = iota(x.shape, 0) % 8
    left = jnp.where(row < 2, x, 0.0)
    right = jnp.where(row >= 2, x, 0.0)
    return jnp.concatenate([left, right], axis=1).astype(BF16)


def own_half(x):
    row = iota((x.shape[0], HD), 0) % 8
    return jnp.where(row < 2, x[:, :HD], x[:, HD:])


def layer_kernel(
    hidden, pre_gain, qw, kw, vw, ow, q_gain, k_gain, post_gain, tk, tv, pos, ik, iv, owner, slot, count,
    out,
    hid_v, pre_v, qw_v, kw_v, vw_v, ow_v, qg_v, kg_v, post_v, tk_v, tv_v, pos_v, ik_v, iv_v, own_v, slot_v, cnt_v,
    q_rows, q_send, q_recv, s_text, o_text, m_text, l_text, s_img, o_img, back_send, back_recv,
    proj, rs_send, rs_recv, ss_send, ss_recv,
    small_sem, load_sem, q_ssem, q_rsem, b_ssem, b_rsem, r_ssem, r_rsem, s_ssem, s_rsem,
):
    g = lax.axis_index("grp")
    h = lax.axis_index("head")

    small = [
        (hidden, hid_v),
        (pre_gain, pre_v),
        (q_gain, qg_v),
        (k_gain, kg_v),
        (post_gain, post_v),
        (pos, pos_v),
        (owner, own_v),
        (slot, slot_v),
        (count, cnt_v),
    ]
    small_copies = [pltpu.make_async_copy(a, b, small_sem.at[i]) for i, (a, b) in enumerate(small)]
    loads = []
    started = [0]

    def load(src, dst):
        loads.append(pltpu.make_async_copy(src, dst, load_sem.at[len(loads)]))
        return len(loads) - 1

    def start_loads(until):
        for i in range(started[0], min(until, len(loads))):
            loads[i].start()
        started[0] = max(started[0], min(until, len(loads)))

    def arrived(i):
        start_loads(i + 1)
        loads[i].wait()
        start_loads(i + 1 + IN_FLIGHT)

    q_loads = [load(qw.at[pl.ds(c, Q_CHUNK)], qw_v.at[pl.ds(c, Q_CHUNK)]) for c in range(0, D, Q_CHUNK)]
    k_loads = [load(kw.at[pl.ds(c, KV_CHUNK)], kw_v.at[pl.ds(c, KV_CHUNK)]) for c in range(0, D, KV_CHUNK)]
    v_loads = [load(vw.at[pl.ds(c, KV_CHUNK)], vw_v.at[pl.ds(c, KV_CHUNK)]) for c in range(0, D, KV_CHUNK)]
    ik_loads = [load(ik.at[pl.ds(j, IMG_STEP)], ik_v.at[pl.ds(j, IMG_STEP)]) for j in range(0, SLOTS, IMG_STEP)]
    iv_loads = [load(iv.at[pl.ds(j, IMG_STEP)], iv_v.at[pl.ds(j, IMG_STEP)]) for j in range(0, SLOTS, IMG_STEP)]
    tk_loads = [load(tk.at[pl.ds(b, TEXT_STEP)], tk_v.at[pl.ds(b, TEXT_STEP)]) for b in range(0, ROWS, TEXT_STEP)]
    tv_loads = [load(tv.at[pl.ds(b, TEXT_STEP)], tv_v.at[pl.ds(b, TEXT_STEP)]) for b in range(0, ROWS, TEXT_STEP)]
    o_loads = [load(ow.at[:, pl.ds(c, OW_CHUNK)], ow_v.at[:, pl.ds(c, OW_CHUNK)]) for c in range(0, D, OW_CHUNK)]
    for copy in small_copies:
        copy.start()
    start_loads(IN_FLIGHT)

    barrier = pltpu.get_barrier_semaphore()
    for k in range(1, GROUPS):
        pl.semaphore_signal(barrier, inc=1, device_id={"grp": (g + k) % GROUPS})
    for k in range(1, HEADS):
        pl.semaphore_signal(barrier, inc=1, device_id={"head": (h + k) % HEADS})

    for copy in small_copies:
        copy.wait()

    x = hid_v[...].astype(F32)
    mean_sq = jnp.mean(x * x, axis=-1, keepdims=True)
    inverse = lax.rsqrt(mean_sq + EPS)
    normed = jnp.concatenate(
        [x[:, i * HD : (i + 1) * HD] * inverse * pre_v[pl.ds(i, 1), :] for i in range(D // HD)], axis=1
    ).astype(BF16)

    lane = iota((ROWS, HD), 1)
    pos_col = jnp.sum(
        jnp.where(iota((ROWS, ROWS), 0) == iota((ROWS, ROWS), 1), pos_v[...].astype(F32), 0.0), axis=1, keepdims=True
    )
    freq = jnp.exp(-math.log(BASE) * (lane % 64).astype(F32) / 64.0)
    angle = pos_col * freq
    cosine = jnp.cos(angle)
    sine = jnp.where(lane < 64, -jnp.sin(angle), jnp.sin(angle))

    def head_norm(v, gain):
        ms = jnp.mean(v * v, axis=-1, keepdims=True)
        v = v * lax.rsqrt(ms + EPS) * gain
        return v * cosine + pltpu.roll(v, 64, 1) * sine

    acc = jnp.zeros((ROWS, QHEADS * HD), F32)
    for i, index in enumerate(q_loads):
        arrived(index)
        c = i * Q_CHUNK
        acc = acc + matmul(normed[:, c : c + Q_CHUNK], qw_v[pl.ds(c, Q_CHUNK), :])
    queries = []
    for i in range(QHEADS):
        q = head_norm(acc[:, i * HD : (i + 1) * HD], qg_v[...]) * (1.0 / math.sqrt(D // QH))
        queries.append(q.astype(BF16).astype(F32))
    for i in range(8):
        q_rows[pl.ds(i * ROWS, ROWS), :] = queries[i] if i < QHEADS else jnp.zeros((ROWS, HD), F32)
    packed = jnp.concatenate(queries, axis=0).astype(BF16)
    q_send[...] = packed
    q_recv[g] = packed

    pl.semaphore_wait(barrier, GROUPS - 1 + HEADS - 1)

    def to_group(k):
        peer = (g + k) % GROUPS
        return pltpu.make_async_remote_copy(
            src_ref=q_send, dst_ref=q_recv.at[g], send_sem=q_ssem.at[k], recv_sem=q_rsem.at[g], device_id={"grp": peer}
        )

    def from_group(k):
        peer = (g + k) % GROUPS
        return pltpu.make_async_remote_copy(
            src_ref=q_send, dst_ref=q_recv.at[peer], send_sem=q_ssem.at[k], recv_sem=q_rsem.at[peer],
            device_id={"grp": peer},
        )

    for k in range(1, GROUPS):
        to_group(k).start()

    k_acc = jnp.zeros((ROWS, KVW), F32)
    v_acc = jnp.zeros((ROWS, KVW), F32)
    for i in range(len(k_loads)):
        c = i * KV_CHUNK
        arrived(k_loads[i])
        k_acc = k_acc + matmul(normed[:, c : c + KV_CHUNK], kw_v[pl.ds(c, KV_CHUNK), :])
    for i in range(len(v_loads)):
        c = i * KV_CHUNK
        arrived(v_loads[i])
        v_acc = v_acc + matmul(normed[:, c : c + KV_CHUNK], vw_v[pl.ds(c, KV_CHUNK), :])
    new_keys = [head_norm(k_acc[:, i * HD : (i + 1) * HD], kg_v[...]).astype(BF16).astype(F32) for i in range(2)]
    new_values = [v_acc[:, i * HD : (i + 1) * HD].astype(BF16).astype(F32) for i in range(2)]
    self_score = [jnp.sum(queries[i] * new_keys[i // 2], axis=-1, keepdims=True) for i in range(QHEADS)]

    code = (own_v[...] * 32 + slot_v[...]).astype(F32)
    counts = cnt_v[...].astype(F32)
    mine = (g * 32).astype(F32)
    n_req = GROUPS * ROWS
    slot_row = mine + (iota((SLOTS * 8, n_req), 0) // 8).astype(F32)
    hit = slot_row == code
    r_row = iota((SLOTS * 8, n_req), 0) % 8
    pick = jnp.concatenate([jnp.where(hit & (r_row == i), 1.0, 0.0) for i in range(QHEADS)], axis=1).astype(BF16)
    slot_count = jnp.sum(jnp.where(hit, counts, 0.0), axis=1, keepdims=True)
    code_col = jnp.sum(
        jnp.where(iota((n_req, n_req), 0) == iota((n_req, n_req), 1), code, 0.0), axis=1, keepdims=True
    )
    slot_lane = mine + (iota((n_req, 256), 1) // 8).astype(F32)
    hit_back = code_col == slot_lane
    r_lane = iota((n_req, 256), 1) % 8
    in_store = iota((n_req, 256), 1) < SLOTS * 8
    put = jnp.concatenate(
        [jnp.where(hit_back & in_store & (r_lane == i), 1.0, 0.0) for i in range(QHEADS)], axis=0
    ).astype(BF16)

    for k in range(1, GROUPS):
        from_group(k).wait_recv()
    pieces = [q_recv[p].astype(F32) for p in range(GROUPS)]
    every = jnp.concatenate(
        [pieces[p][i * ROWS : (i + 1) * ROWS] for i in range(QHEADS) for p in range(GROUPS)], axis=0
    ).astype(BF16)
    asked = block_diagonal(matmul(pick, every))
    for step in range(SLOTS // IMG_STEP):
        arrived(ik_loads[step])
        for j in range(step * IMG_STEP, (step + 1) * IMG_STEP):
            s_img[pl.ds(j * 8, 8), :] = matmul_t(asked[j * 8 : (j + 1) * 8], ik_v[j])
    s = s_img[...]
    valid = iota((SLOTS * 8, IMG), 1).astype(F32) < slot_count
    s = jnp.where(valid, s, NEG)
    top = jnp.max(s, axis=-1, keepdims=True)
    weights = jnp.where(valid, jnp.exp(s - top), 0.0).astype(BF16)
    total = jnp.sum(weights.astype(F32), axis=-1, keepdims=True)
    for step in range(SLOTS // IMG_STEP):
        arrived(iv_loads[step])
        for j in range(step * IMG_STEP, (step + 1) * IMG_STEP):
            o_img[pl.ds(j * 8, 8), :] = own_half(matmul(weights[j * 8 : (j + 1) * 8], iv_v[j]))
    some = total > 0.0
    safe = jnp.where(some, total, 1.0)
    mean_value = (o_img[...] / safe).astype(BF16)
    level = jnp.where(some, top + jnp.log(safe), 0.0)
    high = level.astype(BF16).astype(F32)
    middle = (level - high).astype(BF16).astype(F32)
    low = level - high - middle
    part = iota((SLOTS * 8, HD), 1) % 32 // 8
    right_head = iota((SLOTS * 8, HD), 1) // 32 == iota((SLOTS * 8, HD), 0) % 8
    level_parts = jnp.where(part == 0, high, jnp.where(part == 1, middle, jnp.where(part == 2, low, 0.0)))
    level_parts = jnp.where(right_head, level_parts, 0.0).astype(BF16)
    table = jnp.concatenate([mean_value, level_parts], axis=1)
    table = jnp.concatenate([table, jnp.zeros((256 - SLOTS * 8, 256), BF16)], axis=0)
    back = matmul(put, table)
    for p in range(GROUPS):
        rows = [back[i * n_req + p * ROWS : i * n_req + (p + 1) * ROWS] for i in range(QHEADS)]
        levels = rows[0][:, HD:] + rows[1][:, HD:] + rows[2][:, HD:] + rows[3][:, HD:]
        slab = jnp.concatenate([r[:, :HD] for r in rows] + [levels, jnp.zeros((ROWS, HD), F32)], axis=0)
        back_send[p] = slab.astype(BF16)

    def back_to(k):
        peer = (g + k) % GROUPS
        return pltpu.make_async_remote_copy(
            src_ref=back_send.at[peer], dst_ref=back_recv.at[g], send_sem=b_ssem.at[k], recv_sem=b_rsem.at[g],
            device_id={"grp": peer},
        )

    def back_from(k):
        peer = (g + k) % GROUPS
        return pltpu.make_async_remote_copy(
            src_ref=back_send.at[peer], dst_ref=back_recv.at[peer], send_sem=b_ssem.at[k], recv_sem=b_rsem.at[peer],
            device_id={"grp": peer},
        )

    for k in range(1, GROUPS):
        back_to(k).start()
    back_recv[g] = back_send[g]

    for b in range(ROWS):
        if b % TEXT_STEP == 0:
            arrived(tk_loads[b // TEXT_STEP])
        q = block_diagonal(q_rows[pl.ds(b, 8, stride=8), :])
        s_text[pl.ds(b * 8, 8), :] = matmul_t(q, tk_v[b])
    place = iota((8, WINDOW), 1)
    for b in range(ROWS):
        if b % TEXT_STEP == 0:
            arrived(tv_loads[b // TEXT_STEP])
        p = jnp.sum(jnp.where(iota((8, ROWS), 1) == b, pos_v[...].astype(F32), 0.0), axis=1, keepdims=True)
        p = p.astype(jnp.int32)
        ok = (place < p) & (place != p % WINDOW)
        s = jnp.where(ok, s_text[pl.ds(b * 8, 8), :], NEG)
        top = jnp.max(s, axis=-1, keepdims=True)
        w = jnp.where(ok, jnp.exp(s - top), 0.0).astype(BF16)
        total = jnp.sum(w.astype(F32), axis=-1, keepdims=True)
        o_text[pl.ds(b * 8, 8), :] = own_half(matmul(w, tv_v[b]))
        m_text[pl.ds(b * 8, 8), :] = jnp.broadcast_to(top, (8, HD))
        l_text[pl.ds(b * 8, 8), :] = jnp.broadcast_to(total, (8, HD))

    for k in range(1, GROUPS):
        back_from(k).wait_recv()
    image = back_recv[0].astype(F32)
    for p in range(1, GROUPS):
        image = image + back_recv[p].astype(F32)
    levels = image[QHEADS * ROWS : QHEADS * ROWS + ROWS]
    levels = levels + pltpu.roll(levels, HD - 8, 1) + pltpu.roll(levels, HD - 16, 1)
    attended = []
    for i in range(QHEADS):
        level = jnp.broadcast_to(levels[:, i * 32 : i * 32 + 1], (ROWS, HD))
        mt = m_text[pl.ds(i, ROWS, stride=8), :]
        lt = l_text[pl.ds(i, ROWS, stride=8), :]
        ot = o_text[pl.ds(i, ROWS, stride=8), :]
        own = jnp.broadcast_to(self_score[i], (ROWS, HD))
        top = jnp.maximum(jnp.maximum(level, mt), own)
        from_image = jnp.exp(level - top)
        from_text = jnp.exp(mt - top)
        from_self = jnp.exp(own - top)
        summed = image[i * ROWS : (i + 1) * ROWS] * from_image + ot * from_text + new_values[i // 2] * from_self
        attended.append(summed / (from_image + lt * from_text + from_self))
    attended = jnp.concatenate(attended, axis=1).astype(BF16)

    for i, index in enumerate(o_loads):
        arrived(index)
        cols = pl.ds(i * OW_CHUNK, OW_CHUNK)
        proj[:, cols] = matmul(attended, ow_v[:, cols])
    for p in range(HEADS):
        start, shift = p * WIDTH // 128 * 128, p * WIDTH % 128
        piece = proj[:, pl.ds(start, WIDTH_PAD)]
        rs_send[p] = pltpu.roll(piece, WIDTH_PAD - shift, 1) if shift else piece

    def share_to(k):
        peer = (h + k) % HEADS
        return pltpu.make_async_remote_copy(
            src_ref=rs_send.at[peer], dst_ref=rs_recv.at[h], send_sem=r_ssem.at[k], recv_sem=r_rsem.at[h],
            device_id={"head": peer},
        )

    def share_from(k):
        peer = (h + k) % HEADS
        return pltpu.make_async_remote_copy(
            src_ref=rs_send.at[peer], dst_ref=rs_recv.at[peer], send_sem=r_ssem.at[k], recv_sem=r_rsem.at[peer],
            device_id={"head": peer},
        )

    for k in range(1, HEADS):
        share_to(k).start()

    start = pl.multiple_of(h * WIDTH // 128 * 128, 128)
    aligned = hid_v[:, pl.ds(start, WIDTH_PAD)].astype(F32)
    residual = aligned
    for c in range(1, 4):
        residual = jnp.where(h % 4 == c, pltpu.roll(aligned, WIDTH_PAD - 32 * c, 1), residual)

    share = rs_send[h]
    for k in range(1, HEADS):
        share_from(k).wait_recv()
        share = share + rs_recv[(h + k) % HEADS]
    share = share[:, :WIDTH]
    squares = jnp.broadcast_to(jnp.sum(share * share, axis=-1, keepdims=True), (ROWS, 128))
    ss_send[...] = squares

    def squares_to(k):
        peer = (h + k) % HEADS
        return pltpu.make_async_remote_copy(
            src_ref=ss_send, dst_ref=ss_recv.at[h], send_sem=s_ssem.at[k], recv_sem=s_rsem.at[h],
            device_id={"head": peer},
        )

    def squares_from(k):
        peer = (h + k) % HEADS
        return pltpu.make_async_remote_copy(
            src_ref=ss_send, dst_ref=ss_recv.at[peer], send_sem=s_ssem.at[k], recv_sem=s_rsem.at[peer],
            device_id={"head": peer},
        )

    for k in range(1, HEADS):
        squares_to(k).start()
    for k in range(1, HEADS):
        squares_from(k).wait_recv()
        squares = squares + ss_recv[(h + k) % HEADS]
    scale = lax.rsqrt(squares[:, :1] / D + EPS)
    out[...] = (residual[:, :WIDTH] + share * scale * post_v[...].reshape(1, WIDTH)).astype(BF16)

    for k in range(1, GROUPS):
        to_group(k).wait_send()
        back_to(k).wait_send()
    for k in range(1, HEADS):
        share_to(k).wait_send()
        squares_to(k).wait_send()


def local(*args):
    (hidden, pre_gain, qw, kw, vw, ow, q_gain, k_gain, post_gain, tk, tv, pos, ik, iv, owner, slot, count) = args
    row = lambda v: v.reshape(1, -1)
    operands = [
        hidden, pre_gain.reshape(D // HD, HD), qw, kw, vw, ow, row(q_gain), row(k_gain), post_gain, tk, tv, row(pos), ik, iv,
        row(owner), row(slot), row(count),
    ]
    shapes = [pltpu.VMEM(v.shape, v.dtype) for v in operands]
    dma = pltpu.SemaphoreType.DMA
    n_loads = D // Q_CHUNK + 2 * (D // KV_CHUNK) + D // OW_CHUNK + 2 * (SLOTS // IMG_STEP) + 2 * (ROWS // TEXT_STEP)
    scratch = shapes + [
        pltpu.VMEM((64, HD), F32),
        pltpu.VMEM((QHEADS * ROWS, HD), BF16),
        pltpu.VMEM((GROUPS, QHEADS * ROWS, HD), BF16),
        pltpu.VMEM((ROWS * 8, WINDOW), F32),
        pltpu.VMEM((ROWS * 8, HD), F32),
        pltpu.VMEM((ROWS * 8, HD), F32),
        pltpu.VMEM((ROWS * 8, HD), F32),
        pltpu.VMEM((SLOTS * 8, IMG), F32),
        pltpu.VMEM((SLOTS * 8, HD), F32),
        pltpu.VMEM((GROUPS, 48, HD), BF16),
        pltpu.VMEM((GROUPS, 48, HD), BF16),
        pltpu.VMEM((ROWS, D), F32),
        pltpu.VMEM((HEADS, ROWS, WIDTH_PAD), F32),
        pltpu.VMEM((HEADS, ROWS, WIDTH_PAD), F32),
        pltpu.VMEM((ROWS, 128), F32),
        pltpu.VMEM((HEADS, ROWS, 128), F32),
        dma((9,)),
        dma((n_loads,)),
        dma((GROUPS,)),
        dma((GROUPS,)),
        dma((GROUPS,)),
        dma((GROUPS,)),
        dma((HEADS,)),
        dma((HEADS,)),
        dma((HEADS,)),
        dma((HEADS,)),
    ]
    return pl.pallas_call(
        layer_kernel,
        out_shape=jax.ShapeDtypeStruct((ROWS, WIDTH), BF16),
        in_specs=[pl.BlockSpec(memory_space=pl.ANY)] * len(operands),
        out_specs=pl.BlockSpec(memory_space=pltpu.VMEM),
        scratch_shapes=scratch,
        compiler_params=pltpu.CompilerParams(
            collective_id=0, has_side_effects=True, vmem_limit_bytes=60 * 1024 * 1024
        ),
    )(*operands)


def solution(mesh):
    placed = (
        P("grp", None),
        P(),
        P(None, "head"),
        P(None, "head"),
        P(None, "head"),
        P("head", None),
        P(),
        P(),
        P("head"),
        P("grp", None, "head"),
        P("grp", None, "head"),
        P("grp"),
        P("grp", None, "head"),
        P("grp", None, "head"),
        P(),
        P(),
        P(),
    )
    return jax.shard_map(
        local, mesh=mesh, in_specs=placed, out_specs=P("grp", "head"), check_vma=False
    )
```

```python
import functools
import math

import jax
import jax.numpy as jnp
from jax import lax
from jax.experimental import pallas as pl
from jax.experimental.pallas import tpu as pltpu
from jax.sharding import PartitionSpec as P

D = 5376
QH = 32
HD = 128
EPS = 1e-06
BASE = 1000000.0
F32 = jnp.float32
BF16 = jnp.bfloat16
NEG = -1e30

GROUPS = 16
HEADS = 8
ROWS = 8
QHEADS = 4
KVW = 256
WINDOW = 1024
IMG = 256
SLOTS = 24
WIDTH = D // HEADS
WIDTH_PAD = 768
Q_CHUNK = 1792
KV_CHUNK = 5376
OW_CHUNK = 1792
IMG_STEP = 12
TEXT_STEP = 4
IN_FLIGHT = 4


def iota(shape, dim):
    return lax.broadcasted_iota(jnp.int32, shape, dim)


def matmul(a, b):
    return jnp.dot(a, b, preferred_element_type=F32)


def matmul_t(a, b):
    return lax.dot_general(a, b, (((1,), (1,)), ((), ())), preferred_element_type=F32)


def block_diagonal(x):
    row = iota(x.shape, 0) % 8
    left = jnp.where(row < 2, x, 0.0)
    right = jnp.where(row >= 2, x, 0.0)
    return jnp.concatenate([left, right], axis=1).astype(BF16)


def own_half(x):
    row = iota((x.shape[0], HD), 0) % 8
    return jnp.where(row < 2, x[:, :HD], x[:, HD:])


def layer_kernel(
    hidden, pre_gain, qw, kw, vw, ow, q_gain, k_gain, post_gain, tk, tv, pos, ik, iv, owner, slot, count,
    out,
    hid_v, pre_v, qw_v, kw_v, vw_v, ow_v, gains_v, post_v, tk_v, tv_v, pos_v, ik_v, iv_v, table_v,
    q_rows, q_send, q_recv, s_text, o_text, m_text, l_text, s_img, o_img, back_send, back_recv,
    proj, rs_send, rs_recv, ss_send, ss_recv,
    small_sem, load_sem, sem,
):
    g = lax.axis_index("grp")
    h = lax.axis_index("head")

    small = [
        (hidden, hid_v),
        (pre_gain, pre_v),
        (post_gain, post_v),
        (pos, pos_v),
    ]
    small_copies = [pltpu.make_async_copy(a, b, small_sem.at[i]) for i, (a, b) in enumerate(small)]
    gain_copies = [
        pltpu.make_async_copy(a, gains_v.at[pl.ds(i, 1)], small_sem.at[4]) for i, a in enumerate((q_gain, k_gain))
    ]
    table_copies = [
        pltpu.make_async_copy(a, table_v.at[pl.ds(i, 1)], small_sem.at[5]) for i, a in enumerate((owner, slot, count))
    ]
    loads = []
    started = [0]

    def load(src, dst):
        loads.append(pltpu.make_async_copy(src, dst, load_sem.at[len(loads)]))
        return len(loads) - 1

    def start_loads(until):
        for i in range(started[0], min(until, len(loads))):
            loads[i].start()
        started[0] = max(started[0], min(until, len(loads)))

    def arrived(i):
        start_loads(i + 1)
        loads[i].wait()
        start_loads(i + 1 + IN_FLIGHT)

    q_loads = [load(qw.at[pl.ds(c, Q_CHUNK)], qw_v.at[pl.ds(c, Q_CHUNK)]) for c in range(0, D, Q_CHUNK)]
    k_loads = [load(kw.at[pl.ds(c, KV_CHUNK)], kw_v.at[pl.ds(c, KV_CHUNK)]) for c in range(0, D, KV_CHUNK)]
    v_loads = [load(vw.at[pl.ds(c, KV_CHUNK)], vw_v.at[pl.ds(c, KV_CHUNK)]) for c in range(0, D, KV_CHUNK)]
    ik_loads = [load(ik.at[pl.ds(j, IMG_STEP)], ik_v.at[pl.ds(j, IMG_STEP)]) for j in range(0, SLOTS, IMG_STEP)]
    iv_loads = [load(iv.at[pl.ds(j, IMG_STEP)], iv_v.at[pl.ds(j, IMG_STEP)]) for j in range(0, SLOTS, IMG_STEP)]
    tk_loads = [load(tk.at[pl.ds(b, TEXT_STEP)], tk_v.at[pl.ds(b, TEXT_STEP)]) for b in range(0, ROWS, TEXT_STEP)]
    tv_loads = [load(tv.at[pl.ds(b, TEXT_STEP)], tv_v.at[pl.ds(b, TEXT_STEP)]) for b in range(0, ROWS, TEXT_STEP)]
    o_loads = [load(ow.at[:, pl.ds(c, OW_CHUNK)], ow_v.at[:, pl.ds(c, OW_CHUNK)]) for c in range(0, D, OW_CHUNK)]
    for copy in small_copies + gain_copies + table_copies:
        copy.start()
    start_loads(IN_FLIGHT)

    barrier = pltpu.get_barrier_semaphore()
    for k in range(1, GROUPS):
        pl.semaphore_signal(barrier, inc=1, device_id={"grp": (g + k) % GROUPS})
    for k in range(1, HEADS):
        pl.semaphore_signal(barrier, inc=1, device_id={"head": (h + k) % HEADS})

    for copy in small_copies:
        copy.wait()
    pltpu.make_async_copy(gains_v, gains_v, small_sem.at[4]).wait()
    pltpu.make_async_copy(table_v, table_v, small_sem.at[5]).wait()

    x = hid_v[...].astype(F32)
    mean_sq = jnp.mean(x * x, axis=-1, keepdims=True)
    inverse = lax.rsqrt(mean_sq + EPS)
    normed = jnp.concatenate(
        [x[:, i * HD : (i + 1) * HD] * inverse * pre_v[pl.ds(i, 1), :] for i in range(D // HD)], axis=1
    ).astype(BF16)

    lane = iota((ROWS, HD), 1)
    pos_col = jnp.sum(
        jnp.where(iota((ROWS, ROWS), 0) == iota((ROWS, ROWS), 1), pos_v[...].astype(F32), 0.0), axis=1, keepdims=True
    )
    freq = jnp.exp(-math.log(BASE) * (lane % 64).astype(F32) / 64.0)
    angle = pos_col * freq
    cosine = jnp.cos(angle)
    sine = jnp.where(lane < 64, -jnp.sin(angle), jnp.sin(angle))

    def head_norm(v, gain):
        ms = jnp.mean(v * v, axis=-1, keepdims=True)
        v = v * lax.rsqrt(ms + EPS) * gain
        return v * cosine + pltpu.roll(v, 64, 1) * sine

    acc = jnp.zeros((ROWS, QHEADS * HD), F32)
    for i, index in enumerate(q_loads):
        arrived(index)
        c = i * Q_CHUNK
        acc = acc + matmul(normed[:, c : c + Q_CHUNK], qw_v[pl.ds(c, Q_CHUNK), :])
    queries = []
    for i in range(QHEADS):
        q = head_norm(acc[:, i * HD : (i + 1) * HD], gains_v[pl.ds(0, 1), :]) * (1.0 / math.sqrt(D // QH))
        queries.append(q.astype(BF16).astype(F32))
    for i in range(8):
        q_rows[pl.ds(i * ROWS, ROWS), :] = queries[i] if i < QHEADS else jnp.zeros((ROWS, HD), F32)
    packed = jnp.concatenate(queries, axis=0).astype(BF16)
    q_send[...] = packed
    q_recv[g] = packed

    pl.semaphore_wait(barrier, GROUPS - 1 + HEADS - 1)

    def exchange(axis, me, size, source, target, pair):
        copies = []
        for k in range(1, size):
            peer = (me + k) % size
            copies.append(
                pltpu.make_async_remote_copy(
                    src_ref=source(peer), dst_ref=target.at[me], send_sem=sem.at[pair], recv_sem=sem.at[pair + 1],
                    device_id={axis: peer},
                )
            )
        for copy in copies:
            copy.start()
        whole = target.at[pl.ds(0, size - 1)]
        return pltpu.make_async_remote_copy(
            src_ref=whole, dst_ref=whole, send_sem=sem.at[pair], recv_sem=sem.at[pair + 1],
            device_id={axis: (me + 1) % size},
        )

    asking = exchange("grp", g, GROUPS, lambda peer: q_send, q_recv, 0)

    k_acc = jnp.zeros((ROWS, KVW), F32)
    v_acc = jnp.zeros((ROWS, KVW), F32)
    for i in range(len(k_loads)):
        c = i * KV_CHUNK
        arrived(k_loads[i])
        k_acc = k_acc + matmul(normed[:, c : c + KV_CHUNK], kw_v[pl.ds(c, KV_CHUNK), :])
    for i in range(len(v_loads)):
        c = i * KV_CHUNK
        arrived(v_loads[i])
        v_acc = v_acc + matmul(normed[:, c : c + KV_CHUNK], vw_v[pl.ds(c, KV_CHUNK), :])
    new_keys = [head_norm(k_acc[:, i * HD : (i + 1) * HD], gains_v[pl.ds(1, 1), :]).astype(BF16).astype(F32) for i in range(2)]
    new_values = [v_acc[:, i * HD : (i + 1) * HD].astype(BF16).astype(F32) for i in range(2)]
    self_score = [jnp.sum(queries[i] * new_keys[i // 2], axis=-1, keepdims=True) for i in range(QHEADS)]

    code = (table_v[pl.ds(0, 1), :] * 32 + table_v[pl.ds(1, 1), :]).astype(F32)
    counts = table_v[pl.ds(2, 1), :].astype(F32)
    mine = (g * 32).astype(F32)
    n_req = GROUPS * ROWS
    slot_row = mine + (iota((SLOTS * 8, n_req), 0) // 8).astype(F32)
    hit = slot_row == code
    r_row = iota((SLOTS * 8, n_req), 0) % 8
    pick = jnp.concatenate([jnp.where(hit & (r_row == i), 1.0, 0.0) for i in range(QHEADS)], axis=1).astype(BF16)
    slot_count = jnp.sum(jnp.where(hit, counts, 0.0), axis=1, keepdims=True)
    code_col = jnp.sum(
        jnp.where(iota((n_req, n_req), 0) == iota((n_req, n_req), 1), code, 0.0), axis=1, keepdims=True
    )
    slot_lane = mine + (iota((n_req, 256), 1) // 8).astype(F32)
    hit_back = code_col == slot_lane
    r_lane = iota((n_req, 256), 1) % 8
    in_store = iota((n_req, 256), 1) < SLOTS * 8
    put = jnp.concatenate(
        [jnp.where(hit_back & in_store & (r_lane == i), 1.0, 0.0) for i in range(QHEADS)], axis=0
    ).astype(BF16)

    asking.wait_recv()
    pieces = [q_recv[p].astype(F32) for p in range(GROUPS)]
    every = jnp.concatenate(
        [pieces[p][i * ROWS : (i + 1) * ROWS] for i in range(QHEADS) for p in range(GROUPS)], axis=0
    ).astype(BF16)
    asked = block_diagonal(matmul(pick, every))
    for step in range(SLOTS // IMG_STEP):
        arrived(ik_loads[step])
        for j in range(step * IMG_STEP, (step + 1) * IMG_STEP):
            s_img[pl.ds(j * 8, 8), :] = matmul_t(asked[j * 8 : (j + 1) * 8], ik_v[j])
    s = s_img[...]
    valid = iota((SLOTS * 8, IMG), 1).astype(F32) < slot_count
    s = jnp.where(valid, s, NEG)
    top = jnp.max(s, axis=-1, keepdims=True)
    weights = jnp.where(valid, jnp.exp(s - top), 0.0).astype(BF16)
    total = jnp.sum(weights.astype(F32), axis=-1, keepdims=True)
    for step in range(SLOTS // IMG_STEP):
        arrived(iv_loads[step])
        for j in range(step * IMG_STEP, (step + 1) * IMG_STEP):
            o_img[pl.ds(j * 8, 8), :] = own_half(matmul(weights[j * 8 : (j + 1) * 8], iv_v[j]))
    some = total > 0.0
    safe = jnp.where(some, total, 1.0)
    mean_value = (o_img[...] / safe).astype(BF16)
    level = jnp.where(some, top + jnp.log(safe), 0.0)
    high = level.astype(BF16).astype(F32)
    middle = (level - high).astype(BF16).astype(F32)
    low = level - high - middle
    part = iota((SLOTS * 8, HD), 1) % 32 // 8
    right_head = iota((SLOTS * 8, HD), 1) // 32 == iota((SLOTS * 8, HD), 0) % 8
    level_parts = jnp.where(part == 0, high, jnp.where(part == 1, middle, jnp.where(part == 2, low, 0.0)))
    level_parts = jnp.where(right_head, level_parts, 0.0).astype(BF16)
    table = jnp.concatenate([mean_value, level_parts], axis=1)
    table = jnp.concatenate([table, jnp.zeros((256 - SLOTS * 8, 256), BF16)], axis=0)
    back = matmul(put, table)
    for p in range(GROUPS):
        rows = [back[i * n_req + p * ROWS : i * n_req + (p + 1) * ROWS] for i in range(QHEADS)]
        levels = rows[0][:, HD:] + rows[1][:, HD:] + rows[2][:, HD:] + rows[3][:, HD:]
        slab = jnp.concatenate([r[:, :HD] for r in rows] + [levels, jnp.zeros((ROWS, HD), F32)], axis=0)
        back_send[p] = slab.astype(BF16)

    answering = exchange("grp", g, GROUPS, lambda peer: back_send.at[peer], back_recv, 2)
    back_recv[g] = back_send[g]

    for b in range(ROWS):
        if b % TEXT_STEP == 0:
            arrived(tk_loads[b // TEXT_STEP])
        q = block_diagonal(q_rows[pl.ds(b, 8, stride=8), :])
        s_text[pl.ds(b * 8, 8), :] = matmul_t(q, tk_v[b])
    place = iota((8, WINDOW), 1)
    for b in range(ROWS):
        if b % TEXT_STEP == 0:
            arrived(tv_loads[b // TEXT_STEP])
        p = jnp.sum(jnp.where(iota((8, ROWS), 1) == b, pos_v[...].astype(F32), 0.0), axis=1, keepdims=True)
        p = p.astype(jnp.int32)
        ok = (place < p) & (place != p % WINDOW)
        s = jnp.where(ok, s_text[pl.ds(b * 8, 8), :], NEG)
        top = jnp.max(s, axis=-1, keepdims=True)
        w = jnp.where(ok, jnp.exp(s - top), 0.0).astype(BF16)
        total = jnp.sum(w.astype(F32), axis=-1, keepdims=True)
        o_text[pl.ds(b * 8, 8), :] = own_half(matmul(w, tv_v[b]))
        m_text[pl.ds(b * 8, 8), :] = jnp.broadcast_to(top, (8, HD))
        l_text[pl.ds(b * 8, 8), :] = jnp.broadcast_to(total, (8, HD))

    answering.wait_recv()
    image = back_recv[0].astype(F32)
    for p in range(1, GROUPS):
        image = image + back_recv[p].astype(F32)
    levels = image[QHEADS * ROWS : QHEADS * ROWS + ROWS]
    levels = levels + pltpu.roll(levels, HD - 8, 1) + pltpu.roll(levels, HD - 16, 1)
    attended = []
    for i in range(QHEADS):
        level = jnp.broadcast_to(levels[:, i * 32 : i * 32 + 1], (ROWS, HD))
        mt = m_text[pl.ds(i, ROWS, stride=8), :]
        lt = l_text[pl.ds(i, ROWS, stride=8), :]
        ot = o_text[pl.ds(i, ROWS, stride=8), :]
        own = jnp.broadcast_to(self_score[i], (ROWS, HD))
        top = jnp.maximum(jnp.maximum(level, mt), own)
        from_image = jnp.exp(level - top)
        from_text = jnp.exp(mt - top)
        from_self = jnp.exp(own - top)
        summed = image[i * ROWS : (i + 1) * ROWS] * from_image + ot * from_text + new_values[i // 2] * from_self
        attended.append(summed / (from_image + lt * from_text + from_self))
    attended = jnp.concatenate(attended, axis=1).astype(BF16)

    for i, index in enumerate(o_loads):
        arrived(index)
        cols = pl.ds(i * OW_CHUNK, OW_CHUNK)
        proj[:, cols] = matmul(attended, ow_v[:, cols])
    for p in range(HEADS):
        start, shift = p * WIDTH // 128 * 128, p * WIDTH % 128
        piece = proj[:, pl.ds(start, WIDTH_PAD)]
        rs_send[p] = pltpu.roll(piece, WIDTH_PAD - shift, 1) if shift else piece

    sharing = exchange("head", h, HEADS, lambda peer: rs_send.at[peer], rs_recv, 4)
    rs_recv[h] = rs_send[h]

    start = pl.multiple_of(h * WIDTH // 128 * 128, 128)
    aligned = hid_v[:, pl.ds(start, WIDTH_PAD)].astype(F32)
    residual = aligned
    for c in range(1, 4):
        residual = jnp.where(h % 4 == c, pltpu.roll(aligned, WIDTH_PAD - 32 * c, 1), residual)

    sharing.wait_recv()
    share = rs_recv[0]
    for p in range(1, HEADS):
        share = share + rs_recv[p]
    share = share[:, :WIDTH]
    own_squares = jnp.broadcast_to(jnp.sum(share * share, axis=-1, keepdims=True), (ROWS, 128))
    ss_send[...] = own_squares
    squaring = exchange("head", h, HEADS, lambda peer: ss_send, ss_recv, 6)
    ss_recv[h] = own_squares
    squaring.wait_recv()
    squares = ss_recv[0]
    for p in range(1, HEADS):
        squares = squares + ss_recv[p]
    scale = lax.rsqrt(squares[:, :1] / D + EPS)
    out[...] = (residual[:, :WIDTH] + share * scale * post_v[...].reshape(1, WIDTH)).astype(BF16)

    for whole in (asking, answering, sharing, squaring):
        whole.wait_send()


def local(*args):
    (hidden, pre_gain, qw, kw, vw, ow, q_gain, k_gain, post_gain, tk, tv, pos, ik, iv, owner, slot, count) = args
    row = lambda v: v.reshape(1, -1)
    operands = [
        hidden, pre_gain.reshape(D // HD, HD), qw, kw, vw, ow, row(q_gain), row(k_gain), post_gain, tk, tv, row(pos), ik, iv,
        row(owner), row(slot), row(count),
    ]
    shapes = [pltpu.VMEM(v.shape, v.dtype) for v in operands[:14]]
    shapes[6:8] = [pltpu.VMEM((2, HD), F32)]
    shapes.append(pltpu.VMEM((3, HD), jnp.int32))
    dma = pltpu.SemaphoreType.DMA
    n_loads = D // Q_CHUNK + 2 * (D // KV_CHUNK) + D // OW_CHUNK + 2 * (SLOTS // IMG_STEP) + 2 * (ROWS // TEXT_STEP)
    scratch = shapes + [
        pltpu.VMEM((64, HD), F32),
        pltpu.VMEM((QHEADS * ROWS, HD), BF16),
        pltpu.VMEM((GROUPS, QHEADS * ROWS, HD), BF16),
        pltpu.VMEM((ROWS * 8, WINDOW), F32),
        pltpu.VMEM((ROWS * 8, HD), F32),
        pltpu.VMEM((ROWS * 8, HD), F32),
        pltpu.VMEM((ROWS * 8, HD), F32),
        pltpu.VMEM((SLOTS * 8, IMG), F32),
        pltpu.VMEM((SLOTS * 8, HD), F32),
        pltpu.VMEM((GROUPS, 48, HD), BF16),
        pltpu.VMEM((GROUPS, 48, HD), BF16),
        pltpu.VMEM((ROWS, D), F32),
        pltpu.VMEM((HEADS, ROWS, WIDTH_PAD), F32),
        pltpu.VMEM((HEADS, ROWS, WIDTH_PAD), F32),
        pltpu.VMEM((ROWS, 128), F32),
        pltpu.VMEM((HEADS, ROWS, 128), F32),
        dma((6,)),
        dma((n_loads,)),
        dma((8,)),
    ]
    return pl.pallas_call(
        layer_kernel,
        out_shape=jax.ShapeDtypeStruct((ROWS, WIDTH), BF16),
        in_specs=[pl.BlockSpec(memory_space=pl.ANY)] * len(operands),
        out_specs=pl.BlockSpec(memory_space=pltpu.VMEM),
        scratch_shapes=scratch,
        compiler_params=pltpu.CompilerParams(
            collective_id=0, has_side_effects=True, vmem_limit_bytes=60 * 1024 * 1024
        ),
    )(*operands)


def solution(mesh):
    placed = (
        P("grp", None),
        P(),
        P(None, "head"),
        P(None, "head"),
        P(None, "head"),
        P("head", None),
        P(),
        P(),
        P("head"),
        P("grp", None, "head"),
        P("grp", None, "head"),
        P("grp"),
        P("grp", None, "head"),
        P("grp", None, "head"),
        P(),
        P(),
        P(),
    )
    return jax.shard_map(
        local, mesh=mesh, in_specs=placed, out_specs=P("grp", "head"), check_vma=False
    )
```

```python
import functools
import math

import jax
import jax.numpy as jnp
from jax import lax
from jax.experimental import pallas as pl
from jax.experimental.pallas import tpu as pltpu
from jax.sharding import PartitionSpec as P

D = 5376
QH = 32
HD = 128
EPS = 1e-06
BASE = 1000000.0
F32 = jnp.float32
BF16 = jnp.bfloat16
NEG = -1e30
SHARE = F32

GROUPS = 16
HEADS = 8
ROWS = 8
QHEADS = 4
KVW = 256
WINDOW = 1024
IMG = 256
SLOTS = 24
WIDTH = D // HEADS
WIDTH_PAD = 768
Q_CHUNK = 1792
KV_CHUNK = 5376
OW_CHUNK = 2688
IMG_STEP = 12
TEXT_STEP = 4
FIRST_LOADS = 3
IN_FLIGHT = 4


def iota(shape, dim):
    return lax.broadcasted_iota(jnp.int32, shape, dim)


def matmul(a, b):
    return jnp.dot(a, b, preferred_element_type=F32)


def matmul_t(a, b):
    return lax.dot_general(a, b, (((1,), (1,)), ((), ())), preferred_element_type=F32)


def block_diagonal(x):
    row = iota(x.shape, 0) % 8
    left = jnp.where(row < 2, x, 0.0)
    right = jnp.where(row >= 2, x, 0.0)
    return jnp.concatenate([left, right], axis=1).astype(BF16)


def own_half(x):
    row = iota((x.shape[0], HD), 0) % 8
    return jnp.where(row < 2, x[:, :HD], x[:, HD:])


def layer_kernel(
    hidden, pre_gain, qw, kw, vw, ow, q_gain, k_gain, post_gain, tk, tv, pos, ik, iv, owner, slot, count,
    out,
    hid_v, pre_v, qw_v, kw_v, vw_v, ow_v, gains_v, post_v, tk_v, tv_v, pos_v, ik_v, iv_v, table_v,
    q_rows, q_send, q_recv, s_text, o_text, m_text, l_text, s_img, o_img, back_send, back_recv,
    proj, rs_send, rs_recv, ss_send, ss_recv,
    small_sem, load_sem, sem,
):
    g = lax.axis_index("grp")
    h = lax.axis_index("head")

    z, y_hi, core = g // 4, g // 2 % 2, g % 2
    y_lo, x_at = h // 4, h % 4
    steps = [(a, b, c) for a in range(4) for b in range(2) for c in range(2) if a + b + c > 0]
    steps.sort(key=lambda t: -(10 * min(t[0], 4 - t[0]) + 20 * t[1] + t[2]))
    group_peers = [(z + a) % 4 * 4 + (y_hi + b) % 2 * 2 + (core + c) % 2 for a, b, c in steps]
    other_half = (y_lo + 1) % 2 * 4
    far_heads = [other_half + (x_at + a) % 4 for a in (2, 1, 3, 0)]
    near_heads = [y_lo * 4 + (x_at + a) % 4 for a in (2, 1, 3)]
    head_peers = far_heads + near_heads

    small = [
        (hidden, hid_v),
        (pre_gain, pre_v),
        (post_gain, post_v),
        (pos, pos_v),
    ]
    small_copies = [pltpu.make_async_copy(a, b, small_sem.at[i]) for i, (a, b) in enumerate(small)]
    gain_copies = [
        pltpu.make_async_copy(a, gains_v.at[pl.ds(i, 1)], small_sem.at[4]) for i, a in enumerate((q_gain, k_gain))
    ]
    table_copies = [
        pltpu.make_async_copy(a, table_v.at[pl.ds(i, 1)], small_sem.at[5]) for i, a in enumerate((owner, slot, count))
    ]
    loads = []
    started = [0]

    def load(src, dst):
        loads.append(pltpu.make_async_copy(src, dst, load_sem.at[len(loads)]))
        return len(loads) - 1

    def start_loads(until):
        for i in range(started[0], min(until, len(loads))):
            loads[i].start()
        started[0] = max(started[0], min(until, len(loads)))

    def arrived(i):
        start_loads(i + 1)
        loads[i].wait()
        start_loads(i + 1 + IN_FLIGHT)

    q_loads = [load(qw.at[pl.ds(c, Q_CHUNK)], qw_v.at[pl.ds(c, Q_CHUNK)]) for c in range(0, D, Q_CHUNK)]
    k_loads = [load(kw.at[pl.ds(c, KV_CHUNK)], kw_v.at[pl.ds(c, KV_CHUNK)]) for c in range(0, D, KV_CHUNK)]
    v_loads = [load(vw.at[pl.ds(c, KV_CHUNK)], vw_v.at[pl.ds(c, KV_CHUNK)]) for c in range(0, D, KV_CHUNK)]
    ik_loads = [load(ik.at[pl.ds(j, IMG_STEP)], ik_v.at[pl.ds(j, IMG_STEP)]) for j in range(0, SLOTS, IMG_STEP)]
    iv_loads = [load(iv.at[pl.ds(j, IMG_STEP)], iv_v.at[pl.ds(j, IMG_STEP)]) for j in range(0, SLOTS, IMG_STEP)]
    tk_loads = [load(tk.at[pl.ds(b, TEXT_STEP)], tk_v.at[pl.ds(b, TEXT_STEP)]) for b in range(0, ROWS, TEXT_STEP)]
    tv_loads = [load(tv.at[pl.ds(b, TEXT_STEP)], tv_v.at[pl.ds(b, TEXT_STEP)]) for b in range(0, ROWS, TEXT_STEP)]
    o_loads = [load(ow.at[:, pl.ds(c, OW_CHUNK)], ow_v.at[:, pl.ds(c, OW_CHUNK)]) for c in range(0, D, OW_CHUNK)]
    for copy in small_copies + gain_copies + table_copies:
        copy.start()
    start_loads(FIRST_LOADS)

    barrier = pltpu.get_barrier_semaphore()
    for peer in group_peers:
        pl.semaphore_signal(barrier, inc=1, device_id={"grp": peer})
    for peer in head_peers:
        pl.semaphore_signal(barrier, inc=1, device_id={"head": peer})

    for copy in small_copies:
        copy.wait()
    pltpu.make_async_copy(gains_v, gains_v, small_sem.at[4]).wait()
    pltpu.make_async_copy(table_v, table_v, small_sem.at[5]).wait()

    x = hid_v[...].astype(F32)
    mean_sq = jnp.mean(x * x, axis=-1, keepdims=True)
    inverse = lax.rsqrt(mean_sq + EPS)
    normed = jnp.concatenate(
        [x[:, i * HD : (i + 1) * HD] * inverse * pre_v[pl.ds(i, 1), :] for i in range(D // HD)], axis=1
    ).astype(BF16)

    lane = iota((ROWS, HD), 1)
    pos_col = jnp.sum(
        jnp.where(iota((ROWS, ROWS), 0) == iota((ROWS, ROWS), 1), pos_v[...].astype(F32), 0.0), axis=1, keepdims=True
    )
    freq = jnp.exp(-math.log(BASE) * (lane % 64).astype(F32) / 64.0)
    angle = pos_col * freq
    cosine = jnp.cos(angle)
    sine = jnp.where(lane < 64, -jnp.sin(angle), jnp.sin(angle))

    def head_norm(v, gain):
        ms = jnp.mean(v * v, axis=-1, keepdims=True)
        v = v * lax.rsqrt(ms + EPS) * gain
        return v * cosine + pltpu.roll(v, 64, 1) * sine

    acc = jnp.zeros((ROWS, QHEADS * HD), F32)
    for i, index in enumerate(q_loads):
        arrived(index)
        c = i * Q_CHUNK
        acc = acc + matmul(normed[:, c : c + Q_CHUNK], qw_v[pl.ds(c, Q_CHUNK), :])
    queries = []
    for i in range(QHEADS):
        q = head_norm(acc[:, i * HD : (i + 1) * HD], gains_v[pl.ds(0, 1), :]) * (1.0 / math.sqrt(D // QH))
        queries.append(q.astype(BF16).astype(F32))
    for i in range(8):
        q_rows[pl.ds(i * ROWS, ROWS), :] = queries[i] if i < QHEADS else jnp.zeros((ROWS, HD), F32)
    packed = jnp.concatenate(queries, axis=0).astype(BF16)
    q_send[...] = packed
    q_recv[g] = packed

    pl.semaphore_wait(barrier, GROUPS - 1 + HEADS - 1)

    def send(axis, me, peers, source, target, pair):
        copies = [
            pltpu.make_async_remote_copy(
                src_ref=source(peer), dst_ref=target.at[me], send_sem=sem.at[pair], recv_sem=sem.at[pair + 1],
                device_id={axis: peer},
            )
            for peer in peers
        ]
        for copy in copies:
            copy.start()

    def everything(axis, peers, target, pair):
        whole = target.at[pl.ds(0, len(peers))]
        return pltpu.make_async_remote_copy(
            src_ref=whole, dst_ref=whole, send_sem=sem.at[pair], recv_sem=sem.at[pair + 1], device_id={axis: peers[0]}
        )

    send("grp", g, group_peers, lambda peer: q_send, q_recv, 0)
    asking = everything("grp", group_peers, q_recv, 0)

    k_acc = jnp.zeros((ROWS, KVW), F32)
    v_acc = jnp.zeros((ROWS, KVW), F32)
    for i in range(len(k_loads)):
        c = i * KV_CHUNK
        arrived(k_loads[i])
        k_acc = k_acc + matmul(normed[:, c : c + KV_CHUNK], kw_v[pl.ds(c, KV_CHUNK), :])
    for i in range(len(v_loads)):
        c = i * KV_CHUNK
        arrived(v_loads[i])
        v_acc = v_acc + matmul(normed[:, c : c + KV_CHUNK], vw_v[pl.ds(c, KV_CHUNK), :])
    new_keys = [head_norm(k_acc[:, i * HD : (i + 1) * HD], gains_v[pl.ds(1, 1), :]).astype(BF16).astype(F32) for i in range(2)]
    new_values = [v_acc[:, i * HD : (i + 1) * HD].astype(BF16).astype(F32) for i in range(2)]
    self_score = [jnp.sum(queries[i] * new_keys[i // 2], axis=-1, keepdims=True) for i in range(QHEADS)]

    code = (table_v[pl.ds(0, 1), :] * 32 + table_v[pl.ds(1, 1), :]).astype(F32)
    counts = table_v[pl.ds(2, 1), :].astype(F32)
    mine = (g * 32).astype(F32)
    n_req = GROUPS * ROWS
    slot_row = mine + (iota((SLOTS * 8, n_req), 0) // 8).astype(F32)
    hit = slot_row == code
    r_row = iota((SLOTS * 8, n_req), 0) % 8
    pick = jnp.concatenate([jnp.where(hit & (r_row == i), 1.0, 0.0) for i in range(QHEADS)], axis=1).astype(BF16)
    slot_count = jnp.sum(jnp.where(hit, counts, 0.0), axis=1, keepdims=True)
    code_col = jnp.sum(
        jnp.where(iota((n_req, n_req), 0) == iota((n_req, n_req), 1), code, 0.0), axis=1, keepdims=True
    )
    slot_lane = mine + (iota((n_req, 256), 1) // 8).astype(F32)
    hit_back = code_col == slot_lane
    r_lane = iota((n_req, 256), 1) % 8
    in_store = iota((n_req, 256), 1) < SLOTS * 8
    put = jnp.concatenate(
        [jnp.where(hit_back & in_store & (r_lane == i), 1.0, 0.0) for i in range(QHEADS)], axis=0
    ).astype(BF16)

    asking.wait_recv()
    pieces = [q_recv[p].astype(F32) for p in range(GROUPS)]
    every = jnp.concatenate(
        [pieces[p][i * ROWS : (i + 1) * ROWS] for i in range(QHEADS) for p in range(GROUPS)], axis=0
    ).astype(BF16)
    asked = block_diagonal(matmul(pick, every))
    for step in range(SLOTS // IMG_STEP):
        arrived(ik_loads[step])
        for j in range(step * IMG_STEP, (step + 1) * IMG_STEP):
            s_img[pl.ds(j * 8, 8), :] = matmul_t(asked[j * 8 : (j + 1) * 8], ik_v[j])
    s = s_img[...]
    valid = iota((SLOTS * 8, IMG), 1).astype(F32) < slot_count
    s = jnp.where(valid, s, NEG)
    top = jnp.max(s, axis=-1, keepdims=True)
    weights = jnp.where(valid, jnp.exp(s - top), 0.0).astype(BF16)
    total = jnp.sum(weights.astype(F32), axis=-1, keepdims=True)
    for step in range(SLOTS // IMG_STEP):
        arrived(iv_loads[step])
        for j in range(step * IMG_STEP, (step + 1) * IMG_STEP):
            o_img[pl.ds(j * 8, 8), :] = own_half(matmul(weights[j * 8 : (j + 1) * 8], iv_v[j]))
    some = total > 0.0
    safe = jnp.where(some, total, 1.0)
    mean_value = (o_img[...] / safe).astype(BF16)
    level = jnp.where(some, top + jnp.log(safe), 0.0)
    high = level.astype(BF16).astype(F32)
    middle = (level - high).astype(BF16).astype(F32)
    low = level - high - middle
    part = iota((SLOTS * 8, HD), 1) % 32 // 8
    right_head = iota((SLOTS * 8, HD), 1) // 32 == iota((SLOTS * 8, HD), 0) % 8
    level_parts = jnp.where(part == 0, high, jnp.where(part == 1, middle, jnp.where(part == 2, low, 0.0)))
    level_parts = jnp.where(right_head, level_parts, 0.0).astype(BF16)
    table = jnp.concatenate([mean_value, level_parts], axis=1)
    table = jnp.concatenate([table, jnp.zeros((256 - SLOTS * 8, 256), BF16)], axis=0)
    back = matmul(put, table)
    for p in range(GROUPS):
        rows = [back[i * n_req + p * ROWS : i * n_req + (p + 1) * ROWS] for i in range(QHEADS)]
        levels = rows[0][:, HD:] + rows[1][:, HD:] + rows[2][:, HD:] + rows[3][:, HD:]
        slab = jnp.concatenate([r[:, :HD] for r in rows] + [levels, jnp.zeros((ROWS, HD), F32)], axis=0)
        back_send[p] = slab.astype(BF16)

    send("grp", g, group_peers, lambda peer: back_send.at[peer], back_recv, 2)
    answering = everything("grp", group_peers, back_recv, 2)
    back_recv[g] = back_send[g]

    for b in range(ROWS):
        if b % TEXT_STEP == 0:
            arrived(tk_loads[b // TEXT_STEP])
        q = block_diagonal(q_rows[pl.ds(b, 8, stride=8), :])
        s_text[pl.ds(b * 8, 8), :] = matmul_t(q, tk_v[b])
    place = iota((8, WINDOW), 1)
    for b in range(ROWS):
        if b % TEXT_STEP == 0:
            arrived(tv_loads[b // TEXT_STEP])
        p = jnp.sum(jnp.where(iota((8, ROWS), 1) == b, pos_v[...].astype(F32), 0.0), axis=1, keepdims=True)
        p = p.astype(jnp.int32)
        ok = (place < p) & (place != p % WINDOW)
        s = jnp.where(ok, s_text[pl.ds(b * 8, 8), :], NEG)
        top = jnp.max(s, axis=-1, keepdims=True)
        w = jnp.where(ok, jnp.exp(s - top), 0.0).astype(BF16)
        total = jnp.sum(w.astype(F32), axis=-1, keepdims=True)
        o_text[pl.ds(b * 8, 8), :] = own_half(matmul(w, tv_v[b]))
        m_text[pl.ds(b * 8, 8), :] = jnp.broadcast_to(top, (8, HD))
        l_text[pl.ds(b * 8, 8), :] = jnp.broadcast_to(total, (8, HD))

    answering.wait_recv()
    image = back_recv[0].astype(F32)
    for p in range(1, GROUPS):
        image = image + back_recv[p].astype(F32)
    levels = image[QHEADS * ROWS : QHEADS * ROWS + ROWS]
    levels = levels + pltpu.roll(levels, HD - 8, 1) + pltpu.roll(levels, HD - 16, 1)
    attended = []
    for i in range(QHEADS):
        level = jnp.broadcast_to(levels[:, i * 32 : i * 32 + 1], (ROWS, HD))
        mt = m_text[pl.ds(i, ROWS, stride=8), :]
        lt = l_text[pl.ds(i, ROWS, stride=8), :]
        ot = o_text[pl.ds(i, ROWS, stride=8), :]
        own = jnp.broadcast_to(self_score[i], (ROWS, HD))
        top = jnp.maximum(jnp.maximum(level, mt), own)
        from_image = jnp.exp(level - top)
        from_text = jnp.exp(mt - top)
        from_self = jnp.exp(own - top)
        summed = image[i * ROWS : (i + 1) * ROWS] * from_image + ot * from_text + new_values[i // 2] * from_self
        attended.append(summed / (from_image + lt * from_text + from_self))
    attended = jnp.concatenate(attended, axis=1).astype(BF16)

    for index in o_loads:
        arrived(index)
    half_width = D // 2
    for half, peers in (((y_lo + 1) % 2, far_heads), (y_lo, near_heads)):
        proj[...] = matmul(attended, ow_v[:, pl.ds(pl.multiple_of(half * half_width, HD), half_width)])
        for i in range(HEADS // 2):
            start, shift = i * WIDTH // HD * HD, i * WIDTH % HD
            piece = proj[:, pl.ds(start, WIDTH_PAD)]
            rs_send[half * 4 + i] = (pltpu.roll(piece, WIDTH_PAD - shift, 1) if shift else piece).astype(SHARE)
        send("head", h, peers, lambda peer: rs_send.at[peer], rs_recv, 4)
    sharing = everything("head", head_peers, rs_recv, 4)
    rs_recv[h] = rs_send[h]

    start = pl.multiple_of(h * WIDTH // 128 * 128, 128)
    aligned = hid_v[:, pl.ds(start, WIDTH_PAD)].astype(F32)
    residual = aligned
    for c in range(1, 4):
        residual = jnp.where(h % 4 == c, pltpu.roll(aligned, WIDTH_PAD - 32 * c, 1), residual)

    sharing.wait_recv()
    share = rs_recv[0].astype(F32)
    for p in range(1, HEADS):
        share = share + rs_recv[p].astype(F32)
    share = share[:, :WIDTH]
    own_squares = jnp.broadcast_to(jnp.sum(share * share, axis=-1, keepdims=True), (ROWS, 128))
    ss_send[...] = own_squares
    send("head", h, head_peers, lambda peer: ss_send, ss_recv, 6)
    squaring = everything("head", head_peers, ss_recv, 6)
    ss_recv[h] = own_squares
    squaring.wait_recv()
    squares = ss_recv[0]
    for p in range(1, HEADS):
        squares = squares + ss_recv[p]
    scale = lax.rsqrt(squares[:, :1] / D + EPS)
    out[...] = (residual[:, :WIDTH] + share * scale * post_v[...].reshape(1, WIDTH)).astype(BF16)

    for whole in (asking, answering, sharing, squaring):
        whole.wait_send()


def local(*args):
    (hidden, pre_gain, qw, kw, vw, ow, q_gain, k_gain, post_gain, tk, tv, pos, ik, iv, owner, slot, count) = args
    row = lambda v: v.reshape(1, -1)
    operands = [
        hidden, pre_gain.reshape(D // HD, HD), qw, kw, vw, ow, row(q_gain), row(k_gain), post_gain, tk, tv, row(pos), ik, iv,
        row(owner), row(slot), row(count),
    ]
    shapes = [pltpu.VMEM(v.shape, v.dtype) for v in operands[:14]]
    shapes[6:8] = [pltpu.VMEM((2, HD), F32)]
    shapes.append(pltpu.VMEM((3, HD), jnp.int32))
    dma = pltpu.SemaphoreType.DMA
    n_loads = D // Q_CHUNK + 2 * (D // KV_CHUNK) + D // OW_CHUNK + 2 * (SLOTS // IMG_STEP) + 2 * (ROWS // TEXT_STEP)
    scratch = shapes + [
        pltpu.VMEM((64, HD), F32),
        pltpu.VMEM((QHEADS * ROWS, HD), BF16),
        pltpu.VMEM((GROUPS, QHEADS * ROWS, HD), BF16),
        pltpu.VMEM((ROWS * 8, WINDOW), F32),
        pltpu.VMEM((ROWS * 8, HD), F32),
        pltpu.VMEM((ROWS * 8, HD), F32),
        pltpu.VMEM((ROWS * 8, HD), F32),
        pltpu.VMEM((SLOTS * 8, IMG), F32),
        pltpu.VMEM((SLOTS * 8, HD), F32),
        pltpu.VMEM((GROUPS, 48, HD), BF16),
        pltpu.VMEM((GROUPS, 48, HD), BF16),
        pltpu.VMEM((ROWS, D // 2), F32),
        pltpu.VMEM((HEADS, ROWS, WIDTH_PAD), SHARE),
        pltpu.VMEM((HEADS, ROWS, WIDTH_PAD), SHARE),
        pltpu.VMEM((ROWS, 128), F32),
        pltpu.VMEM((HEADS, ROWS, 128), F32),
        dma((6,)),
        dma((n_loads,)),
        dma((8,)),
    ]
    return pl.pallas_call(
        layer_kernel,
        out_shape=pltpu.VMEM((ROWS, WIDTH), BF16),
        in_specs=[pl.BlockSpec(memory_space=pl.ANY)] * len(operands),
        out_specs=pl.BlockSpec(memory_space=pltpu.VMEM),
        scratch_shapes=scratch,
        compiler_params=pltpu.CompilerParams(
            collective_id=0, has_side_effects=True, vmem_limit_bytes=60 * 1024 * 1024
        ),
    )(*operands)


def solution(mesh):
    placed = (
        P("grp", None),
        P(),
        P(None, "head"),
        P(None, "head"),
        P(None, "head"),
        P("head", None),
        P(),
        P(),
        P("head"),
        P("grp", None, "head"),
        P("grp", None, "head"),
        P("grp"),
        P("grp", None, "head"),
        P("grp", None, "head"),
        P(),
        P(),
        P(),
    )
    return jax.shard_map(
        local, mesh=mesh, in_specs=placed, out_specs=P("grp", "head"), check_vma=False
    )
```

```python
import functools
import math

import jax
import jax.numpy as jnp
from jax import lax
from jax.experimental import pallas as pl
from jax.experimental.pallas import tpu as pltpu
from jax.sharding import PartitionSpec as P

D = 5376
QH = 32
HD = 128
EPS = 1e-06
BASE = 1000000.0
F32 = jnp.float32
BF16 = jnp.bfloat16
NEG = -1e30
SHARE = F32

GROUPS = 16
HEADS = 8
ROWS = 8
QHEADS = 4
KVW = 256
WINDOW = 1024
IMG = 256
SLOTS = 24
WIDTH = D // HEADS
WIDTH_PAD = 768
Q_CHUNKS = (768, 1536, 3072)
KV_CHUNK = 5376
OW_CHUNK = 2688
IMG_STEP = 12
IMG_GROUP = 12
TEXT_STEP = 4
FIRST_LOADS = 3
IN_FLIGHT = 5


def iota(shape, dim):
    return lax.broadcasted_iota(jnp.int32, shape, dim)


def matmul(a, b):
    return jnp.dot(a, b, preferred_element_type=F32)


def matmul_t(a, b):
    return lax.dot_general(a, b, (((1,), (1,)), ((), ())), preferred_element_type=F32)


def block_diagonal(x):
    row = iota(x.shape, 0) % 8
    left = jnp.where(row < 2, x, 0.0)
    right = jnp.where(row >= 2, x, 0.0)
    return jnp.concatenate([left, right], axis=1).astype(BF16)


def own_half(x):
    row = iota((x.shape[0], HD), 0) % 8
    return jnp.where(row < 2, x[:, :HD], x[:, HD:])


def layer_kernel(
    hidden, pre_gain, qw, kw, vw, ow, q_gain, k_gain, post_gain, tk, tv, pos, ik, iv, owner, slot, count,
    out,
    hid_v, pre_v, qw_v, kw_v, vw_v, ow_v, gains_v, post_v, tk_v, tv_v, pos_v, ik_v, iv_v, table_v,
    q_rows, q_send, q_recv, s_text, o_text, m_text, l_text, ik_t, back_send, back_recv,
    rs_send, rs_recv, ss_send, ss_recv,
    small_sem, load_sem, sem,
):
    g = lax.axis_index("grp")
    h = lax.axis_index("head")

    z = g // 4
    y_hi = (g - 4 * z) // 2
    core = g - 4 * z - 2 * y_hi
    y_lo = h // 4
    x_at = h - 4 * y_lo
    ring_z = [4 * z] + [4 * lax.rem(z + a, 4) for a in (1, 2, 3)]
    ring_x = [x_at] + [lax.rem(x_at + a, 4) for a in (1, 2, 3)]
    pair_y = [2 * y_hi, 2 - 2 * y_hi]
    pair_core = [core, 1 - core]
    steps = [(a, b, c) for a in range(4) for b in range(2) for c in range(2) if a + b + c > 0]
    steps.sort(key=lambda t: -(10 * min(t[0], 4 - t[0]) + 20 * t[1] + t[2]))
    group_peers = [ring_z[a] + (pair_y[b] + pair_core[c]) for a, b, c in steps]
    far_row, near_row = 4 - 4 * y_lo, 4 * y_lo
    head_peers = [far_row + ring_x[a] for a in (2, 1, 3, 0)] + [near_row + ring_x[a] for a in (2, 1, 3)]

    small = [
        (hidden, hid_v),
        (pre_gain, pre_v),
        (post_gain, post_v),
        (pos, pos_v),
    ]
    small_copies = [pltpu.make_async_copy(a, b, small_sem.at[i]) for i, (a, b) in enumerate(small)]
    gain_copies = [
        pltpu.make_async_copy(a, gains_v.at[pl.ds(i, 1)], small_sem.at[4]) for i, a in enumerate((q_gain, k_gain))
    ]
    table_copies = [
        pltpu.make_async_copy(a, table_v.at[pl.ds(i, 1)], small_sem.at[5]) for i, a in enumerate((owner, slot, count))
    ]
    loads = []
    started = [0]

    def load(src, dst):
        loads.append(pltpu.make_async_copy(src, dst, load_sem.at[len(loads)]))
        return len(loads) - 1

    def start_loads(until):
        for i in range(started[0], min(until, len(loads))):
            loads[i].start()
        started[0] = max(started[0], min(until, len(loads)))

    def arrived(i):
        start_loads(i + 1)
        loads[i].wait()
        start_loads(i + 1 + IN_FLIGHT)

    q_starts = [sum(Q_CHUNKS[:i]) for i in range(len(Q_CHUNKS))]
    q_loads = [load(qw.at[pl.ds(c, n)], qw_v.at[pl.ds(c, n)]) for c, n in zip(q_starts, Q_CHUNKS)]
    ik_loads = [load(ik.at[pl.ds(j, IMG_STEP)], ik_v.at[pl.ds(j, IMG_STEP)]) for j in range(0, SLOTS, IMG_STEP)]
    k_loads = [load(kw.at[pl.ds(c, KV_CHUNK)], kw_v.at[pl.ds(c, KV_CHUNK)]) for c in range(0, D, KV_CHUNK)]
    v_loads = [load(vw.at[pl.ds(c, KV_CHUNK)], vw_v.at[pl.ds(c, KV_CHUNK)]) for c in range(0, D, KV_CHUNK)]
    iv_loads = [load(iv.at[pl.ds(j, IMG_STEP)], iv_v.at[pl.ds(j, IMG_STEP)]) for j in range(0, SLOTS, IMG_STEP)]
    tk_loads = [load(tk.at[pl.ds(b, TEXT_STEP)], tk_v.at[pl.ds(b, TEXT_STEP)]) for b in range(0, ROWS, TEXT_STEP)]
    tv_loads = [load(tv.at[pl.ds(b, TEXT_STEP)], tv_v.at[pl.ds(b, TEXT_STEP)]) for b in range(0, ROWS, TEXT_STEP)]
    o_loads = [load(ow.at[:, pl.ds(c, OW_CHUNK)], ow_v.at[:, pl.ds(c, OW_CHUNK)]) for c in range(0, D, OW_CHUNK)]
    for copy in small_copies + gain_copies + table_copies:
        copy.start()
    start_loads(FIRST_LOADS)

    barrier = pltpu.get_barrier_semaphore()
    for peer in group_peers:
        pl.semaphore_signal(barrier, inc=1, device_id={"grp": peer})
    for peer in head_peers:
        pl.semaphore_signal(barrier, inc=1, device_id={"head": peer})

    for copy in small_copies:
        copy.wait()
    pltpu.make_async_copy(gains_v, gains_v, small_sem.at[4]).wait()
    pltpu.make_async_copy(table_v, table_v, small_sem.at[5]).wait()

    x = hid_v[...].astype(F32)
    mean_sq = jnp.mean(x * x, axis=-1, keepdims=True)
    inverse = lax.rsqrt(mean_sq + EPS)
    normed = jnp.concatenate(
        [x[:, i * HD : (i + 1) * HD] * inverse * pre_v[pl.ds(i, 1), :] for i in range(D // HD)], axis=1
    ).astype(BF16)

    lane = iota((ROWS, HD), 1)
    pos_col = jnp.sum(
        jnp.where(iota((ROWS, ROWS), 0) == iota((ROWS, ROWS), 1), pos_v[...].astype(F32), 0.0), axis=1, keepdims=True
    )
    freq = jnp.exp(-math.log(BASE) * (lane % 64).astype(F32) / 64.0)
    angle = pos_col * freq
    cosine = jnp.cos(angle)
    sine = jnp.where(lane < 64, -jnp.sin(angle), jnp.sin(angle))

    def head_norm(v, gain):
        ms = jnp.mean(v * v, axis=-1, keepdims=True)
        v = v * lax.rsqrt(ms + EPS) * gain
        return v * cosine + pltpu.roll(v, 64, 1) * sine

    acc = jnp.zeros((ROWS, QHEADS * HD), F32)
    for index, c, n in zip(q_loads, q_starts, Q_CHUNKS):
        arrived(index)
        acc = acc + matmul(normed[:, c : c + n], qw_v[pl.ds(c, n), :])
    queries = []
    for i in range(QHEADS):
        q = head_norm(acc[:, i * HD : (i + 1) * HD], gains_v[pl.ds(0, 1), :]) * (1.0 / math.sqrt(D // QH))
        queries.append(q.astype(BF16).astype(F32))
    for i in range(8):
        q_rows[pl.ds(i * ROWS, ROWS), :] = queries[i] if i < QHEADS else jnp.zeros((ROWS, HD), F32)
    packed = jnp.concatenate(queries, axis=0).astype(BF16)
    q_send[...] = packed
    q_recv[g] = packed

    pl.semaphore_wait(barrier, GROUPS - 1 + HEADS - 1)

    def send(axis, me, peers, source, target, pair):
        copies = [
            pltpu.make_async_remote_copy(
                src_ref=source(peer), dst_ref=target.at[me], send_sem=sem.at[pair], recv_sem=sem.at[pair + 1],
                device_id={axis: peer},
            )
            for peer in peers
        ]
        for copy in copies:
            copy.start()

    def everything(axis, peers, target, pair):
        whole = target.at[pl.ds(0, len(peers))]
        return pltpu.make_async_remote_copy(
            src_ref=whole, dst_ref=whole, send_sem=sem.at[pair], recv_sem=sem.at[pair + 1], device_id={axis: peers[0]}
        )

    send("grp", g, group_peers, lambda peer: q_send, q_recv, 0)
    asking = everything("grp", group_peers, q_recv, 0)

    code = (table_v[pl.ds(0, 1), :] * 32 + table_v[pl.ds(1, 1), :]).astype(F32)
    counts = table_v[pl.ds(2, 1), :].astype(F32)
    mine = (g * 32).astype(F32)
    n_req = GROUPS * ROWS
    slot_row = mine + (iota((SLOTS * 8, n_req), 0) // 8).astype(F32)
    hit = slot_row == code
    slot_count = jnp.sum(jnp.where(hit, counts, 0.0), axis=1, keepdims=True)
    n_ask = GROUPS * QHEADS * ROWS
    table_row = iota((8, n_req), 0)
    both = jnp.where(table_row == 0, table_v[pl.ds(0, 1), :].astype(F32), table_v[pl.ds(1, 1), :].astype(F32))
    column = iota((n_req, n_ask), 1)
    spread = jnp.where(iota((n_req, n_ask), 0) == column // 32 * 8 + column % 8, 1.0, 0.0).astype(BF16)
    wide = matmul(both.astype(BF16), spread)
    wide_code = wide[0:1] * 32.0 + wide[1:2]
    ask_row = iota((SLOTS * 8, n_ask), 0)
    same_head = iota((SLOTS * 8, n_ask), 1) // 8 % 4 == ask_row % 8
    pick = jnp.where((mine + (ask_row // 8).astype(F32) == wide_code) & same_head, 1.0, 0.0).astype(BF16)
    code_col = jnp.sum(
        jnp.where(iota((n_req, n_req), 0) == iota((n_req, n_req), 1), code, 0.0), axis=1, keepdims=True
    )
    slot_lane = mine + (iota((n_req, 256), 1) // 8).astype(F32)
    hit_back = code_col == slot_lane
    r_lane = iota((n_req, 256), 1) % 8
    in_store = iota((n_req, 256), 1) < SLOTS * 8
    put = jnp.concatenate(
        [jnp.where(hit_back & in_store & (r_lane == i), 1.0, 0.0) for i in range(QHEADS)], axis=0
    ).astype(BF16)

    for step in range(SLOTS // IMG_STEP):
        arrived(ik_loads[step])
        for j in range(step * IMG_STEP, (step + 1) * IMG_STEP):
            ik_t[j] = ik_v[j].T

    k_acc = jnp.zeros((ROWS, KVW), F32)
    v_acc = jnp.zeros((ROWS, KVW), F32)
    for i in range(len(k_loads)):
        c = i * KV_CHUNK
        arrived(k_loads[i])
        k_acc = k_acc + matmul(normed[:, c : c + KV_CHUNK], kw_v[pl.ds(c, KV_CHUNK), :])
    for i in range(len(v_loads)):
        c = i * KV_CHUNK
        arrived(v_loads[i])
        v_acc = v_acc + matmul(normed[:, c : c + KV_CHUNK], vw_v[pl.ds(c, KV_CHUNK), :])
    new_keys = [head_norm(k_acc[:, i * HD : (i + 1) * HD], gains_v[pl.ds(1, 1), :]).astype(BF16).astype(F32) for i in range(2)]
    new_values = [v_acc[:, i * HD : (i + 1) * HD].astype(BF16).astype(F32) for i in range(2)]
    self_score = [jnp.sum(queries[i] * new_keys[i // 2], axis=-1, keepdims=True) for i in range(QHEADS)]

    for index in iv_loads:
        arrived(index)
    asking.wait_recv()
    asked = block_diagonal(matmul(pick, q_recv[...].reshape(n_ask, HD)))
    totals, tops, sums = [], [], []
    for first in range(0, SLOTS, IMG_GROUP):
        slots = range(first, first + IMG_GROUP)
        s = jnp.concatenate([matmul(asked[j * 8 : (j + 1) * 8], ik_t[j]) for j in slots], axis=0)
        valid = iota((IMG_GROUP * 8, IMG), 1).astype(F32) < slot_count[first * 8 : (first + IMG_GROUP) * 8]
        s = jnp.where(valid, s, NEG)
        top = jnp.max(s, axis=-1, keepdims=True)
        weights = jnp.where(valid, jnp.exp(s - top), 0.0).astype(BF16)
        tops.append(top)
        totals.append(jnp.sum(weights.astype(F32), axis=-1, keepdims=True))
        at = lambda j: (j - first) * 8
        sums += [own_half(matmul(weights[at(j) : at(j) + 8], iv_v[j])) for j in slots]
    total = jnp.concatenate(totals, axis=0)
    top = jnp.concatenate(tops, axis=0)
    some = total > 0.0
    safe = jnp.where(some, total, 1.0)
    mean_value = (jnp.concatenate(sums, axis=0) / safe).astype(BF16)
    level = jnp.where(some, top + jnp.log(safe), 0.0)
    high = level.astype(BF16).astype(F32)
    middle = (level - high).astype(BF16).astype(F32)
    low = level - high - middle
    part = iota((SLOTS * 8, HD), 1) % 32 // 8
    right_head = iota((SLOTS * 8, HD), 1) // 32 == iota((SLOTS * 8, HD), 0) % 8
    level_parts = jnp.where(part == 0, high, jnp.where(part == 1, middle, jnp.where(part == 2, low, 0.0)))
    level_parts = jnp.where(right_head, level_parts, 0.0).astype(BF16)
    table = jnp.concatenate([mean_value, level_parts], axis=1)
    table = jnp.concatenate([table, jnp.zeros((256 - SLOTS * 8, 256), BF16)], axis=0)
    back = matmul(put, table)
    for p in range(GROUPS):
        rows = [back[i * n_req + p * ROWS : i * n_req + (p + 1) * ROWS] for i in range(QHEADS)]
        levels = rows[0][:, HD:] + rows[1][:, HD:] + rows[2][:, HD:] + rows[3][:, HD:]
        slab = jnp.concatenate([r[:, :HD] for r in rows] + [levels, jnp.zeros((ROWS, HD), F32)], axis=0)
        back_send[p] = slab.astype(BF16)

    send("grp", g, group_peers, lambda peer: back_send.at[peer], back_recv, 2)
    answering = everything("grp", group_peers, back_recv, 2)
    back_recv[g] = back_send[g]

    for b in range(ROWS):
        if b % TEXT_STEP == 0:
            arrived(tk_loads[b // TEXT_STEP])
        q = block_diagonal(q_rows[pl.ds(b, 8, stride=8), :])
        s_text[pl.ds(b * 8, 8), :] = matmul_t(q, tk_v[b])
    place = iota((8, WINDOW), 1)
    for b in range(ROWS):
        if b % TEXT_STEP == 0:
            arrived(tv_loads[b // TEXT_STEP])
        p = jnp.sum(jnp.where(iota((8, ROWS), 1) == b, pos_v[...].astype(F32), 0.0), axis=1, keepdims=True)
        p = p.astype(jnp.int32)
        ok = (place < p) & (place != p % WINDOW)
        s = jnp.where(ok, s_text[pl.ds(b * 8, 8), :], NEG)
        top = jnp.max(s, axis=-1, keepdims=True)
        w = jnp.where(ok, jnp.exp(s - top), 0.0).astype(BF16)
        total = jnp.sum(w.astype(F32), axis=-1, keepdims=True)
        o_text[pl.ds(b * 8, 8), :] = own_half(matmul(w, tv_v[b]))
        m_text[pl.ds(b * 8, 8), :] = jnp.broadcast_to(top, (8, HD))
        l_text[pl.ds(b * 8, 8), :] = jnp.broadcast_to(total, (8, HD))

    rest = []
    for i in range(QHEADS):
        mt = m_text[pl.ds(i, ROWS, stride=8), :]
        lt = l_text[pl.ds(i, ROWS, stride=8), :]
        ot = o_text[pl.ds(i, ROWS, stride=8), :]
        own = jnp.broadcast_to(self_score[i], (ROWS, HD))
        top = jnp.maximum(mt, own)
        from_text = jnp.exp(mt - top)
        from_self = jnp.exp(own - top)
        rest.append((top, lt * from_text + from_self, ot * from_text + new_values[i // 2] * from_self))
    answering.wait_recv()
    image = back_recv[0].astype(F32)
    for p in range(1, GROUPS):
        image = image + back_recv[p].astype(F32)
    levels = image[QHEADS * ROWS : QHEADS * ROWS + ROWS]
    levels = levels + pltpu.roll(levels, HD - 8, 1) + pltpu.roll(levels, HD - 16, 1)
    attended = []
    for i in range(QHEADS):
        level = jnp.broadcast_to(levels[:, i * 32 : i * 32 + 1], (ROWS, HD))
        rest_top, rest_total, rest_sum = rest[i]
        top = jnp.maximum(level, rest_top)
        from_image = jnp.exp(level - top)
        from_rest = jnp.exp(rest_top - top)
        summed = image[i * ROWS : (i + 1) * ROWS] * from_image + rest_sum * from_rest
        attended.append(summed / (from_image + rest_total * from_rest))
    attended = jnp.concatenate(attended, axis=1).astype(BF16)

    for index in o_loads:
        arrived(index)
    half_width = D // 2
    pair_width = 1408
    pair_far = ring_x[2] // 2
    mate = 1 - 2 * (x_at - 2 * (x_at // 2))
    across = [ring_x[2], ring_x[2] + mate]
    for row, near in ((far_row, [x_at + mate, x_at]), (near_row, [x_at + mate])):
        for pair, peers in ((pair_far, across), (1 - pair_far, near)):
            start = row // 4 * half_width + pair * 1280
            part = matmul(attended, ow_v[:, pl.ds(pl.multiple_of(start, HD), pair_width)])
            for i in range(2):
                piece = part[:, i * 640 : i * 640 + WIDTH_PAD]
                low = pltpu.roll(piece, WIDTH_PAD - 32 * i, 1) if i else piece
                high = pltpu.roll(piece, WIDTH_PAD - 32 * i - 64, 1)
                rs_send[row + 2 * pair + i] = jnp.where(pair == 1, high, low).astype(SHARE)
            send("head", h, [row + x for x in peers], lambda peer: rs_send.at[peer], rs_recv, 4)
    sharing = everything("head", head_peers, rs_recv, 4)
    rs_recv[h] = rs_send[h]

    start = pl.multiple_of(h * WIDTH // 128 * 128, 128)
    aligned = hid_v[:, pl.ds(start, WIDTH_PAD)].astype(F32)
    residual = aligned
    for c in range(1, 4):
        residual = jnp.where(h % 4 == c, pltpu.roll(aligned, WIDTH_PAD - 32 * c, 1), residual)

    sharing.wait_recv()
    share = rs_recv[0].astype(F32)
    for p in range(1, HEADS):
        share = share + rs_recv[p].astype(F32)
    share = share[:, :WIDTH]
    own_squares = jnp.broadcast_to(jnp.sum(share * share, axis=-1, keepdims=True), (ROWS, 128))
    ss_send[...] = own_squares
    send("head", h, head_peers, lambda peer: ss_send, ss_recv, 6)
    squaring = everything("head", head_peers, ss_recv, 6)
    ss_recv[h] = own_squares
    squaring.wait_recv()
    squares = ss_recv[0]
    for p in range(1, HEADS):
        squares = squares + ss_recv[p]
    scale = lax.rsqrt(squares[:, :1] / D + EPS)
    out[...] = (residual[:, :WIDTH] + share * scale * post_v[...].reshape(1, WIDTH)).astype(BF16)

    for whole in (asking, answering, sharing, squaring):
        whole.wait_send()


def local(*args):
    (hidden, pre_gain, qw, kw, vw, ow, q_gain, k_gain, post_gain, tk, tv, pos, ik, iv, owner, slot, count) = args
    row = lambda v: v.reshape(1, -1)
    operands = [
        hidden, pre_gain.reshape(D // HD, HD), qw, kw, vw, ow, row(q_gain), row(k_gain), post_gain, tk, tv, row(pos), ik, iv,
        row(owner), row(slot), row(count),
    ]
    shapes = [pltpu.VMEM(v.shape, v.dtype) for v in operands[:14]]
    shapes[6:8] = [pltpu.VMEM((2, HD), F32)]
    shapes.append(pltpu.VMEM((3, HD), jnp.int32))
    dma = pltpu.SemaphoreType.DMA
    n_loads = len(Q_CHUNKS) + 2 * (D // KV_CHUNK) + D // OW_CHUNK + 2 * (SLOTS // IMG_STEP) + 2 * (ROWS // TEXT_STEP)
    scratch = shapes + [
        pltpu.VMEM((64, HD), F32),
        pltpu.VMEM((QHEADS * ROWS, HD), BF16),
        pltpu.VMEM((GROUPS, QHEADS * ROWS, HD), BF16),
        pltpu.VMEM((ROWS * 8, WINDOW), F32),
        pltpu.VMEM((ROWS * 8, HD), F32),
        pltpu.VMEM((ROWS * 8, HD), F32),
        pltpu.VMEM((ROWS * 8, HD), F32),
        pltpu.VMEM((SLOTS, KVW, IMG), BF16),
        pltpu.VMEM((GROUPS, 48, HD), BF16),
        pltpu.VMEM((GROUPS, 48, HD), BF16),
        pltpu.VMEM((HEADS, ROWS, WIDTH_PAD), SHARE),
        pltpu.VMEM((HEADS, ROWS, WIDTH_PAD), SHARE),
        pltpu.VMEM((ROWS, 128), F32),
        pltpu.VMEM((HEADS, ROWS, 128), F32),
        dma((6,)),
        dma((n_loads,)),
        dma((8,)),
    ]
    return pl.pallas_call(
        layer_kernel,
        out_shape=pltpu.VMEM((ROWS, WIDTH), BF16),
        in_specs=[pl.BlockSpec(memory_space=pl.ANY)] * len(operands),
        out_specs=pl.BlockSpec(memory_space=pltpu.VMEM),
        scratch_shapes=scratch,
        compiler_params=pltpu.CompilerParams(
            collective_id=0, has_side_effects=True, vmem_limit_bytes=60 * 1024 * 1024
        ),
    )(*operands)


def solution(mesh):
    placed = (
        P("grp", None),
        P(),
        P(None, "head"),
        P(None, "head"),
        P(None, "head"),
        P("head", None),
        P(),
        P(),
        P("head"),
        P("grp", None, "head"),
        P("grp", None, "head"),
        P("grp"),
        P("grp", None, "head"),
        P("grp", None, "head"),
        P(),
        P(),
        P(),
    )
    return jax.shard_map(
        local, mesh=mesh, in_specs=placed, out_specs=P("grp", "head"), check_vma=False
    )
```

```python
import functools
import math

import jax
import jax.numpy as jnp
from jax import lax
from jax.experimental import pallas as pl
from jax.experimental.pallas import tpu as pltpu
from jax.sharding import PartitionSpec as P

D = 5376
QH = 32
HD = 128
EPS = 1e-06
BASE = 1000000.0
F32 = jnp.float32
BF16 = jnp.bfloat16
NEG = -1e30
SHARE = BF16

GROUPS = 16
HEADS = 8
ROWS = 8
QHEADS = 4
KVW = 256
WINDOW = 1024
IMG = 256
SLOTS = 24
WIDTH = D // HEADS
WIDTH_PAD = 768
Q_CHUNKS = (768, 1536, 3072)
KV_CHUNK = 5376
OW_CHUNK = 2688
IMG_STEP = 12
IMG_GROUP = 24
TEXT_STEP = 4
FIRST_LOADS = 3
IN_FLIGHT = 5


def iota(shape, dim):
    return lax.broadcasted_iota(jnp.int32, shape, dim)


def matmul(a, b):
    return jnp.dot(a, b, preferred_element_type=F32)


def matmul_t(a, b):
    return lax.dot_general(a, b, (((1,), (1,)), ((), ())), preferred_element_type=F32)


def block_diagonal(x):
    row = iota(x.shape, 0) % 8
    left = jnp.where(row < 2, x, 0.0)
    right = jnp.where(row >= 2, x, 0.0)
    return jnp.concatenate([left, right], axis=1).astype(BF16)


def own_half(x):
    row = iota((x.shape[0], HD), 0) % 8
    return jnp.where(row < 2, x[:, :HD], x[:, HD:])


def layer_kernel(
    hidden, pre_gain, qw, kw, vw, ow, q_gain, k_gain, post_gain, tk, tv, pos, ik, iv, owner, slot, count,
    out,
    hid_v, pre_v, qw_v, kw_v, vw_v, ow_v, gains_v, post_v, tk_v, tv_v, pos_v, ik_v, iv_v, table_v,
    q_rows, q_send, q_recv, s_text, o_text, m_text, l_text, ik_t, back_send, back_recv,
    rs_send, rs_recv, ss_send, ss_recv,
    small_sem, load_sem, sem,
):
    g = lax.axis_index("grp")
    h = lax.axis_index("head")

    z = g // 4
    y_hi = (g - 4 * z) // 2
    core = g - 4 * z - 2 * y_hi
    y_lo = h // 4
    x_at = h - 4 * y_lo
    ring_z = [4 * z] + [4 * lax.rem(z + a, 4) for a in (1, 2, 3)]
    ring_x = [x_at] + [lax.rem(x_at + a, 4) for a in (1, 2, 3)]
    pair_y = [2 * y_hi, 2 - 2 * y_hi]
    pair_core = [core, 1 - core]
    steps = [(a, b, c) for a in range(4) for b in range(2) for c in range(2) if a + b + c > 0]
    steps.sort(key=lambda t: -(10 * min(t[0], 4 - t[0]) + 20 * t[1] + t[2]))
    group_peers = [ring_z[a] + (pair_y[b] + pair_core[c]) for a, b, c in steps]
    far_row, near_row = 4 - 4 * y_lo, 4 * y_lo
    head_peers = [far_row + ring_x[a] for a in (2, 1, 3, 0)] + [near_row + ring_x[a] for a in (2, 1, 3)]

    small = [
        (hidden, hid_v),
        (pre_gain, pre_v),
        (post_gain, post_v),
        (pos, pos_v),
    ]
    small_copies = [pltpu.make_async_copy(a, b, small_sem.at[i]) for i, (a, b) in enumerate(small)]
    gain_copies = [
        pltpu.make_async_copy(a, gains_v.at[pl.ds(i, 1)], small_sem.at[4]) for i, a in enumerate((q_gain, k_gain))
    ]
    table_copies = [
        pltpu.make_async_copy(a, table_v.at[pl.ds(i, 1)], small_sem.at[5]) for i, a in enumerate((owner, slot, count))
    ]
    loads = []
    started = [0]

    def load(src, dst):
        loads.append(pltpu.make_async_copy(src, dst, load_sem.at[len(loads)]))
        return len(loads) - 1

    def start_loads(until):
        for i in range(started[0], min(until, len(loads))):
            loads[i].start()
        started[0] = max(started[0], min(until, len(loads)))

    def arrived(i):
        start_loads(i + 1)
        loads[i].wait()
        start_loads(i + 1 + IN_FLIGHT)

    q_starts = [sum(Q_CHUNKS[:i]) for i in range(len(Q_CHUNKS))]
    q_loads = [load(qw.at[pl.ds(c, n)], qw_v.at[pl.ds(c, n)]) for c, n in zip(q_starts, Q_CHUNKS)]
    ik_loads = [load(ik.at[pl.ds(j, IMG_STEP)], ik_v.at[pl.ds(j, IMG_STEP)]) for j in range(0, SLOTS, IMG_STEP)]
    k_loads = [load(kw.at[pl.ds(c, KV_CHUNK)], kw_v.at[pl.ds(c, KV_CHUNK)]) for c in range(0, D, KV_CHUNK)]
    v_loads = [load(vw.at[pl.ds(c, KV_CHUNK)], vw_v.at[pl.ds(c, KV_CHUNK)]) for c in range(0, D, KV_CHUNK)]
    iv_loads = [load(iv.at[pl.ds(j, IMG_STEP)], iv_v.at[pl.ds(j, IMG_STEP)]) for j in range(0, SLOTS, IMG_STEP)]
    tk_loads = [load(tk.at[pl.ds(b, TEXT_STEP)], tk_v.at[pl.ds(b, TEXT_STEP)]) for b in range(0, ROWS, TEXT_STEP)]
    tv_loads = [load(tv.at[pl.ds(b, TEXT_STEP)], tv_v.at[pl.ds(b, TEXT_STEP)]) for b in range(0, ROWS, TEXT_STEP)]
    o_loads = [load(ow.at[:, pl.ds(c, OW_CHUNK)], ow_v.at[:, pl.ds(c, OW_CHUNK)]) for c in range(0, D, OW_CHUNK)]
    for copy in small_copies + gain_copies + table_copies:
        copy.start()
    start_loads(FIRST_LOADS)

    barrier = pltpu.get_barrier_semaphore()
    for peer in group_peers:
        pl.semaphore_signal(barrier, inc=1, device_id={"grp": peer})
    for peer in head_peers:
        pl.semaphore_signal(barrier, inc=1, device_id={"head": peer})

    for copy in small_copies:
        copy.wait()
    pltpu.make_async_copy(gains_v, gains_v, small_sem.at[4]).wait()
    pltpu.make_async_copy(table_v, table_v, small_sem.at[5]).wait()

    x = hid_v[...].astype(F32)
    mean_sq = jnp.mean(x * x, axis=-1, keepdims=True)
    inverse = lax.rsqrt(mean_sq + EPS)
    normed = jnp.concatenate(
        [x[:, i * HD : (i + 1) * HD] * inverse * pre_v[pl.ds(i, 1), :] for i in range(D // HD)], axis=1
    ).astype(BF16)

    lane = iota((ROWS, HD), 1)
    pos_col = jnp.sum(
        jnp.where(iota((ROWS, ROWS), 0) == iota((ROWS, ROWS), 1), pos_v[...].astype(F32), 0.0), axis=1, keepdims=True
    )
    freq = jnp.exp(-math.log(BASE) * (lane % 64).astype(F32) / 64.0)
    angle = pos_col * freq
    cosine = jnp.cos(angle)
    sine = jnp.where(lane < 64, -jnp.sin(angle), jnp.sin(angle))

    def head_norm(v, gain):
        ms = jnp.mean(v * v, axis=-1, keepdims=True)
        v = v * lax.rsqrt(ms + EPS) * gain
        return v * cosine + pltpu.roll(v, 64, 1) * sine

    acc = jnp.zeros((ROWS, QHEADS * HD), F32)
    for index, c, n in zip(q_loads, q_starts, Q_CHUNKS):
        arrived(index)
        acc = acc + matmul(normed[:, c : c + n], qw_v[pl.ds(c, n), :])
    queries = []
    for i in range(QHEADS):
        q = head_norm(acc[:, i * HD : (i + 1) * HD], gains_v[pl.ds(0, 1), :]) * (1.0 / math.sqrt(D // QH))
        queries.append(q.astype(BF16).astype(F32))
    for i in range(8):
        q_rows[pl.ds(i * ROWS, ROWS), :] = queries[i] if i < QHEADS else jnp.zeros((ROWS, HD), F32)
    packed = jnp.concatenate(queries, axis=0).astype(BF16)
    q_send[...] = packed
    q_recv[g] = packed

    pl.semaphore_wait(barrier, GROUPS - 1 + HEADS - 1)

    def send(axis, me, peers, source, target, pair):
        copies = [
            pltpu.make_async_remote_copy(
                src_ref=source(peer), dst_ref=target.at[me], send_sem=sem.at[pair], recv_sem=sem.at[pair + 1],
                device_id={axis: peer},
            )
            for peer in peers
        ]
        for copy in copies:
            copy.start()

    def everything(axis, peers, target, pair):
        whole = target.at[pl.ds(0, len(peers))]
        return pltpu.make_async_remote_copy(
            src_ref=whole, dst_ref=whole, send_sem=sem.at[pair], recv_sem=sem.at[pair + 1], device_id={axis: peers[0]}
        )

    send("grp", g, group_peers, lambda peer: q_send, q_recv, 0)
    asking = everything("grp", group_peers, q_recv, 0)

    code = (table_v[pl.ds(0, 1), :] * 32 + table_v[pl.ds(1, 1), :]).astype(F32)
    counts = table_v[pl.ds(2, 1), :].astype(F32)
    mine = (g * 32).astype(F32)
    n_req = GROUPS * ROWS
    slot_row = mine + (iota((SLOTS * 8, n_req), 0) // 8).astype(F32)
    hit = slot_row == code
    slot_count = jnp.sum(jnp.where(hit, counts, 0.0), axis=1, keepdims=True)
    n_ask = GROUPS * QHEADS * ROWS
    table_row = iota((8, n_req), 0)
    both = jnp.where(table_row == 0, table_v[pl.ds(0, 1), :].astype(F32), table_v[pl.ds(1, 1), :].astype(F32))
    column = iota((n_req, n_ask), 1)
    spread = jnp.where(iota((n_req, n_ask), 0) == column // 32 * 8 + column % 8, 1.0, 0.0).astype(BF16)
    wide = matmul(both.astype(BF16), spread)
    wide_code = wide[0:1] * 32.0 + wide[1:2]
    ask_row = iota((SLOTS * 8, n_ask), 0)
    same_head = iota((SLOTS * 8, n_ask), 1) // 8 % 4 == ask_row % 8
    pick = jnp.where((mine + (ask_row // 8).astype(F32) == wide_code) & same_head, 1.0, 0.0).astype(BF16)
    code_col = jnp.sum(
        jnp.where(iota((n_req, n_req), 0) == iota((n_req, n_req), 1), code, 0.0), axis=1, keepdims=True
    )
    slot_lane = mine + (iota((n_req, 256), 1) // 8).astype(F32)
    hit_back = code_col == slot_lane
    r_lane = iota((n_req, 256), 1) % 8
    in_store = iota((n_req, 256), 1) < SLOTS * 8
    put = jnp.concatenate(
        [jnp.where(hit_back & in_store & (r_lane == i), 1.0, 0.0) for i in range(QHEADS)], axis=0
    ).astype(BF16)

    for step in range(SLOTS // IMG_STEP):
        arrived(ik_loads[step])
        for j in range(step * IMG_STEP, (step + 1) * IMG_STEP):
            ik_t[j] = ik_v[j].T

    k_acc = jnp.zeros((ROWS, KVW), F32)
    v_acc = jnp.zeros((ROWS, KVW), F32)
    for i in range(len(k_loads)):
        c = i * KV_CHUNK
        arrived(k_loads[i])
        k_acc = k_acc + matmul(normed[:, c : c + KV_CHUNK], kw_v[pl.ds(c, KV_CHUNK), :])
    for i in range(len(v_loads)):
        c = i * KV_CHUNK
        arrived(v_loads[i])
        v_acc = v_acc + matmul(normed[:, c : c + KV_CHUNK], vw_v[pl.ds(c, KV_CHUNK), :])
    new_keys = [head_norm(k_acc[:, i * HD : (i + 1) * HD], gains_v[pl.ds(1, 1), :]).astype(BF16).astype(F32) for i in range(2)]
    new_values = [v_acc[:, i * HD : (i + 1) * HD].astype(BF16).astype(F32) for i in range(2)]
    self_score = [jnp.sum(queries[i] * new_keys[i // 2], axis=-1, keepdims=True) for i in range(QHEADS)]

    for index in iv_loads:
        arrived(index)
    asking.wait_recv()
    asked = block_diagonal(matmul(pick, q_recv[...].reshape(n_ask, HD)))
    totals, tops, sums = [], [], []
    for first in range(0, SLOTS, IMG_GROUP):
        slots = range(first, first + IMG_GROUP)
        s = jnp.concatenate([matmul(asked[j * 8 : (j + 1) * 8], ik_t[j]) for j in slots], axis=0)
        valid = iota((IMG_GROUP * 8, IMG), 1).astype(F32) < slot_count[first * 8 : (first + IMG_GROUP) * 8]
        s = jnp.where(valid, s, NEG)
        top = jnp.max(s, axis=-1, keepdims=True)
        weights = jnp.where(valid, jnp.exp(s - top), 0.0).astype(BF16)
        tops.append(top)
        totals.append(jnp.sum(weights.astype(F32), axis=-1, keepdims=True))
        at = lambda j: (j - first) * 8
        sums += [own_half(matmul(weights[at(j) : at(j) + 8], iv_v[j])) for j in slots]
    total = jnp.concatenate(totals, axis=0)
    top = jnp.concatenate(tops, axis=0)
    some = total > 0.0
    safe = jnp.where(some, total, 1.0)
    mean_value = (jnp.concatenate(sums, axis=0) / safe).astype(BF16)
    level = jnp.where(some, top + jnp.log(safe), 0.0)
    high = level.astype(BF16).astype(F32)
    middle = (level - high).astype(BF16).astype(F32)
    low = level - high - middle
    part = iota((SLOTS * 8, HD), 1) % 32 // 8
    right_head = iota((SLOTS * 8, HD), 1) // 32 == iota((SLOTS * 8, HD), 0) % 8
    level_parts = jnp.where(part == 0, high, jnp.where(part == 1, middle, jnp.where(part == 2, low, 0.0)))
    level_parts = jnp.where(right_head, level_parts, 0.0).astype(BF16)
    table = jnp.concatenate([mean_value, level_parts], axis=1)
    table = jnp.concatenate([table, jnp.zeros((256 - SLOTS * 8, 256), BF16)], axis=0)
    back = matmul(put, table)
    for p in range(GROUPS):
        rows = [back[i * n_req + p * ROWS : i * n_req + (p + 1) * ROWS] for i in range(QHEADS)]
        levels = rows[0][:, HD:] + rows[1][:, HD:] + rows[2][:, HD:] + rows[3][:, HD:]
        slab = jnp.concatenate([r[:, :HD] for r in rows] + [levels], axis=0)
        back_send[p] = slab.astype(BF16)

    send("grp", g, group_peers, lambda peer: back_send.at[peer], back_recv, 2)
    answering = everything("grp", group_peers, back_recv, 2)
    back_recv[g] = back_send[g]

    for b in range(ROWS):
        if b % TEXT_STEP == 0:
            arrived(tk_loads[b // TEXT_STEP])
        q = block_diagonal(q_rows[pl.ds(b, 8, stride=8), :])
        s_text[pl.ds(b * 8, 8), :] = matmul_t(q, tk_v[b])
    place = iota((8, WINDOW), 1)
    for b in range(ROWS):
        if b % TEXT_STEP == 0:
            arrived(tv_loads[b // TEXT_STEP])
        p = jnp.sum(jnp.where(iota((8, ROWS), 1) == b, pos_v[...].astype(F32), 0.0), axis=1, keepdims=True)
        p = p.astype(jnp.int32)
        ok = (place < p) & (place != p % WINDOW)
        s = jnp.where(ok, s_text[pl.ds(b * 8, 8), :], NEG)
        top = jnp.max(s, axis=-1, keepdims=True)
        w = jnp.where(ok, jnp.exp(s - top), 0.0).astype(BF16)
        total = jnp.sum(w.astype(F32), axis=-1, keepdims=True)
        o_text[pl.ds(b * 8, 8), :] = own_half(matmul(w, tv_v[b]))
        m_text[pl.ds(b * 8, 8), :] = jnp.broadcast_to(top, (8, HD))
        l_text[pl.ds(b * 8, 8), :] = jnp.broadcast_to(total, (8, HD))

    rest = []
    for i in range(QHEADS):
        mt = m_text[pl.ds(i, ROWS, stride=8), :]
        lt = l_text[pl.ds(i, ROWS, stride=8), :]
        ot = o_text[pl.ds(i, ROWS, stride=8), :]
        own = jnp.broadcast_to(self_score[i], (ROWS, HD))
        top = jnp.maximum(mt, own)
        from_text = jnp.exp(mt - top)
        from_self = jnp.exp(own - top)
        rest.append((top, lt * from_text + from_self, ot * from_text + new_values[i // 2] * from_self))
    answering.wait_recv()
    image = back_recv[0].astype(F32)
    for p in range(1, GROUPS):
        image = image + back_recv[p].astype(F32)
    levels = image[QHEADS * ROWS : QHEADS * ROWS + ROWS]
    levels = levels + pltpu.roll(levels, HD - 8, 1) + pltpu.roll(levels, HD - 16, 1)
    attended = []
    for i in range(QHEADS):
        level = jnp.broadcast_to(levels[:, i * 32 : i * 32 + 1], (ROWS, HD))
        rest_top, rest_total, rest_sum = rest[i]
        top = jnp.maximum(level, rest_top)
        from_image = jnp.exp(level - top)
        from_rest = jnp.exp(rest_top - top)
        summed = image[i * ROWS : (i + 1) * ROWS] * from_image + rest_sum * from_rest
        attended.append(summed / (from_image + rest_total * from_rest))
    attended = jnp.concatenate(attended, axis=1).astype(BF16)

    for index in o_loads:
        arrived(index)
    half_width = D // 2
    pair_width = 1408
    pair_far = ring_x[2] // 2
    mate = 1 - 2 * (x_at - 2 * (x_at // 2))
    across = [ring_x[2], ring_x[2] + mate]
    for row, near in ((far_row, [x_at + mate, x_at]), (near_row, [x_at + mate])):
        for pair, peers in ((pair_far, across), (1 - pair_far, near)):
            start = row // 4 * half_width + pair * 1280
            part = matmul(attended, ow_v[:, pl.ds(pl.multiple_of(start, HD), pair_width)])
            for i in range(2):
                piece = part[:, i * 640 : i * 640 + WIDTH_PAD]
                low = pltpu.roll(piece, WIDTH_PAD - 32 * i, 1) if i else piece
                high = pltpu.roll(piece, WIDTH_PAD - 32 * i - 64, 1)
                rs_send[row + 2 * pair + i] = jnp.where(pair == 1, high, low).astype(SHARE)
            send("head", h, [row + x for x in peers], lambda peer: rs_send.at[peer], rs_recv, 4)
    sharing = everything("head", head_peers, rs_recv, 4)
    rs_recv[h] = rs_send[h]

    start = pl.multiple_of(h * WIDTH // 128 * 128, 128)
    aligned = hid_v[:, pl.ds(start, WIDTH_PAD)].astype(F32)
    residual = aligned
    for c in range(1, 4):
        residual = jnp.where(h % 4 == c, pltpu.roll(aligned, WIDTH_PAD - 32 * c, 1), residual)

    sharing.wait_recv()
    share = rs_recv[0].astype(F32)
    for p in range(1, HEADS):
        share = share + rs_recv[p].astype(F32)
    share = share[:, :WIDTH]
    own_squares = jnp.broadcast_to(jnp.sum(share * share, axis=-1, keepdims=True), (ROWS, 128))
    ss_send[...] = own_squares
    send("head", h, head_peers, lambda peer: ss_send, ss_recv, 6)
    squaring = everything("head", head_peers, ss_recv, 6)
    ss_recv[h] = own_squares
    squaring.wait_recv()
    squares = ss_recv[0]
    for p in range(1, HEADS):
        squares = squares + ss_recv[p]
    scale = lax.rsqrt(squares[:, :1] / D + EPS)
    out[...] = (residual[:, :WIDTH] + share * scale * post_v[...].reshape(1, WIDTH)).astype(BF16)

    for whole in (asking, answering, sharing, squaring):
        whole.wait_send()


def local(*args):
    (hidden, pre_gain, qw, kw, vw, ow, q_gain, k_gain, post_gain, tk, tv, pos, ik, iv, owner, slot, count) = args
    row = lambda v: v.reshape(1, -1)
    operands = [
        hidden, pre_gain.reshape(D // HD, HD), qw, kw, vw, ow, row(q_gain), row(k_gain), post_gain, tk, tv, row(pos), ik, iv,
        row(owner), row(slot), row(count),
    ]
    shapes = [pltpu.VMEM(v.shape, v.dtype) for v in operands[:14]]
    shapes[6:8] = [pltpu.VMEM((2, HD), F32)]
    shapes.append(pltpu.VMEM((3, HD), jnp.int32))
    dma = pltpu.SemaphoreType.DMA
    n_loads = len(Q_CHUNKS) + 2 * (D // KV_CHUNK) + D // OW_CHUNK + 2 * (SLOTS // IMG_STEP) + 2 * (ROWS // TEXT_STEP)
    scratch = shapes + [
        pltpu.VMEM((64, HD), F32),
        pltpu.VMEM((QHEADS * ROWS, HD), BF16),
        pltpu.VMEM((GROUPS, QHEADS * ROWS, HD), BF16),
        pltpu.VMEM((ROWS * 8, WINDOW), F32),
        pltpu.VMEM((ROWS * 8, HD), F32),
        pltpu.VMEM((ROWS * 8, HD), F32),
        pltpu.VMEM((ROWS * 8, HD), F32),
        pltpu.VMEM((SLOTS, KVW, IMG), BF16),
        pltpu.VMEM((GROUPS, 40, HD), BF16),
        pltpu.VMEM((GROUPS, 40, HD), BF16),
        pltpu.VMEM((HEADS, ROWS, WIDTH_PAD), SHARE),
        pltpu.VMEM((HEADS, ROWS, WIDTH_PAD), SHARE),
        pltpu.VMEM((ROWS, 128), F32),
        pltpu.VMEM((HEADS, ROWS, 128), F32),
        dma((6,)),
        dma((n_loads,)),
        dma((8,)),
    ]
    return pl.pallas_call(
        layer_kernel,
        out_shape=pltpu.VMEM((ROWS, WIDTH), BF16),
        in_specs=[pl.BlockSpec(memory_space=pl.ANY)] * len(operands),
        out_specs=pl.BlockSpec(memory_space=pltpu.VMEM),
        scratch_shapes=scratch,
        compiler_params=pltpu.CompilerParams(
            collective_id=0, has_side_effects=True, vmem_limit_bytes=60 * 1024 * 1024
        ),
    )(*operands)


def solution(mesh):
    placed = (
        P("grp", None),
        P(),
        P(None, "head"),
        P(None, "head"),
        P(None, "head"),
        P("head", None),
        P(),
        P(),
        P("head"),
        P("grp", None, "head"),
        P("grp", None, "head"),
        P("grp"),
        P("grp", None, "head"),
        P("grp", None, "head"),
        P(),
        P(),
        P(),
    )
    return jax.shard_map(
        local, mesh=mesh, in_specs=placed, out_specs=P("grp", "head"), check_vma=False
    )
```

```python
import functools
import math

import jax
import jax.numpy as jnp
from jax import lax
from jax.experimental import pallas as pl
from jax.experimental.pallas import tpu as pltpu
from jax.sharding import PartitionSpec as P

D = 5376
QH = 32
HD = 128
EPS = 1e-06
BASE = 1000000.0
F32 = jnp.float32
BF16 = jnp.bfloat16
NEG = -1e30
SHARE = BF16

GROUPS = 16
HEADS = 8
ROWS = 8
QHEADS = 4
KVW = 256
WINDOW = 1024
IMG = 256
SLOTS = 24
WIDTH = D // HEADS
WIDTH_PAD = 768
Q_CHUNKS = (768, 1536, 3072)
KV_CHUNK = 5376
OW_CHUNK = 2688
IMG_STEP = 12
IMG_GROUP = 24
TEXT_STEP = 4
FIRST_LOADS = 3
IN_FLIGHT = 5


def iota(shape, dim):
    return lax.broadcasted_iota(jnp.int32, shape, dim)


def matmul(a, b):
    return jnp.dot(a, b, preferred_element_type=F32)


def matmul_t(a, b):
    return lax.dot_general(a, b, (((1,), (1,)), ((), ())), preferred_element_type=F32)


def block_diagonal(x):
    row = iota(x.shape, 0) % 8
    left = jnp.where(row < 2, x, 0.0)
    right = jnp.where(row >= 2, x, 0.0)
    return jnp.concatenate([left, right], axis=1).astype(BF16)


def own_half(x):
    row = iota((x.shape[0], HD), 0) % 8
    return jnp.where(row < 2, x[:, :HD], x[:, HD:])


def layer_kernel(
    hidden, pre_gain, qw, kw, vw, ow, q_gain, k_gain, post_gain, tk, tv, pos, ik, iv, owner, slot, count,
    out,
    hid_v, pre_v, qw_v, kw_v, vw_v, ow_v, gains_v, post_v, tk_v, tv_v, pos_v, ik_v, iv_v, table_v,
    q_rows, q_send, q_recv, s_text, o_text, m_text, l_text, ik_t, back_send, back_recv,
    rs_send, rs_recv, ss_send, ss_recv,
    small_sem, load_sem, sem,
):
    g = lax.axis_index("grp")
    h = lax.axis_index("head")

    z = g // 4
    y_hi = (g - 4 * z) // 2
    core = g - 4 * z - 2 * y_hi
    y_lo = h // 4
    x_at = h - 4 * y_lo
    ring_z = [4 * z] + [4 * lax.rem(z + a, 4) for a in (1, 2, 3)]
    ring_x = [x_at] + [lax.rem(x_at + a, 4) for a in (1, 2, 3)]
    pair_y = [2 * y_hi, 2 - 2 * y_hi]
    pair_core = [core, 1 - core]
    steps = [(a, b, c) for a in range(4) for b in range(2) for c in range(2) if a + b + c > 0]
    steps.sort(key=lambda t: -(10 * min(t[0], 4 - t[0]) + 20 * t[1] + t[2]))
    group_peers = [ring_z[a] + (pair_y[b] + pair_core[c]) for a, b, c in steps]
    far_row, near_row = 4 - 4 * y_lo, 4 * y_lo
    head_peers = [far_row + ring_x[a] for a in (2, 1, 3, 0)] + [near_row + ring_x[a] for a in (2, 1, 3)]

    small = [
        (hidden, hid_v),
        (pre_gain, pre_v),
        (post_gain, post_v),
        (pos, pos_v),
    ]
    small_copies = [pltpu.make_async_copy(a, b, small_sem.at[i]) for i, (a, b) in enumerate(small)]
    gain_copies = [
        pltpu.make_async_copy(a, gains_v.at[pl.ds(i, 1)], small_sem.at[4]) for i, a in enumerate((q_gain, k_gain))
    ]
    table_copies = [
        pltpu.make_async_copy(a, table_v.at[pl.ds(i, 1)], small_sem.at[5]) for i, a in enumerate((owner, slot, count))
    ]
    loads = []
    started = [0]

    def load(src, dst):
        loads.append(pltpu.make_async_copy(src, dst, load_sem.at[len(loads)]))
        return len(loads) - 1

    def start_loads(until):
        for i in range(started[0], min(until, len(loads))):
            loads[i].start()
        started[0] = max(started[0], min(until, len(loads)))

    def arrived(i):
        start_loads(i + 1)
        loads[i].wait()
        start_loads(i + 1 + IN_FLIGHT)

    q_starts = [sum(Q_CHUNKS[:i]) for i in range(len(Q_CHUNKS))]
    q_loads = [load(qw.at[pl.ds(c, n)], qw_v.at[pl.ds(c, n)]) for c, n in zip(q_starts, Q_CHUNKS)]
    ik_loads = [load(ik.at[pl.ds(j, IMG_STEP)], ik_v.at[pl.ds(j, IMG_STEP)]) for j in range(0, SLOTS, IMG_STEP)]
    k_loads = [load(kw.at[pl.ds(c, KV_CHUNK)], kw_v.at[pl.ds(c, KV_CHUNK)]) for c in range(0, D, KV_CHUNK)]
    v_loads = [load(vw.at[pl.ds(c, KV_CHUNK)], vw_v.at[pl.ds(c, KV_CHUNK)]) for c in range(0, D, KV_CHUNK)]
    iv_loads = [load(iv.at[pl.ds(j, IMG_STEP)], iv_v.at[pl.ds(j, IMG_STEP)]) for j in range(0, SLOTS, IMG_STEP)]
    tk_loads = [load(tk.at[pl.ds(b, TEXT_STEP)], tk_v.at[pl.ds(b, TEXT_STEP)]) for b in range(0, ROWS, TEXT_STEP)]
    tv_loads = [load(tv.at[pl.ds(b, TEXT_STEP)], tv_v.at[pl.ds(b, TEXT_STEP)]) for b in range(0, ROWS, TEXT_STEP)]
    o_loads = [load(ow.at[:, pl.ds(c, OW_CHUNK)], ow_v.at[:, pl.ds(c, OW_CHUNK)]) for c in range(0, D, OW_CHUNK)]
    for copy in small_copies + gain_copies + table_copies:
        copy.start()
    start_loads(FIRST_LOADS)

    barrier = pltpu.get_barrier_semaphore()
    for peer in group_peers:
        pl.semaphore_signal(barrier, inc=1, device_id={"grp": peer})
    for peer in head_peers:
        pl.semaphore_signal(barrier, inc=1, device_id={"head": peer})

    for copy in small_copies:
        copy.wait()
    pltpu.make_async_copy(gains_v, gains_v, small_sem.at[4]).wait()
    pltpu.make_async_copy(table_v, table_v, small_sem.at[5]).wait()

    x = hid_v[...].astype(F32)
    mean_sq = jnp.mean(x * x, axis=-1, keepdims=True)
    inverse = lax.rsqrt(mean_sq + EPS)
    normed = jnp.concatenate(
        [x[:, i * HD : (i + 1) * HD] * inverse * pre_v[pl.ds(i, 1), :] for i in range(D // HD)], axis=1
    ).astype(BF16)

    lane = iota((ROWS, HD), 1)
    pos_col = jnp.sum(
        jnp.where(iota((ROWS, ROWS), 0) == iota((ROWS, ROWS), 1), pos_v[...].astype(F32), 0.0), axis=1, keepdims=True
    )
    freq = jnp.exp(-math.log(BASE) * (lane % 64).astype(F32) / 64.0)
    angle = pos_col * freq
    cosine = jnp.cos(angle)
    sine = jnp.where(lane < 64, -jnp.sin(angle), jnp.sin(angle))

    def head_norm(v, gain):
        ms = jnp.mean(v * v, axis=-1, keepdims=True)
        v = v * lax.rsqrt(ms + EPS) * gain
        return v * cosine + pltpu.roll(v, 64, 1) * sine

    acc = jnp.zeros((ROWS, QHEADS * HD), F32)
    for index, c, n in zip(q_loads, q_starts, Q_CHUNKS):
        arrived(index)
        acc = acc + matmul(normed[:, c : c + n], qw_v[pl.ds(c, n), :])
    queries = []
    for i in range(QHEADS):
        q = head_norm(acc[:, i * HD : (i + 1) * HD], gains_v[pl.ds(0, 1), :]) * (1.0 / math.sqrt(D // QH))
        queries.append(q.astype(BF16).astype(F32))
    for i in range(8):
        q_rows[pl.ds(i * ROWS, ROWS), :] = queries[i] if i < QHEADS else jnp.zeros((ROWS, HD), F32)
    packed = jnp.concatenate(queries, axis=0).astype(BF16)
    q_send[...] = packed
    q_recv[g] = packed

    pl.semaphore_wait(barrier, GROUPS - 1 + HEADS - 1)

    def send(axis, me, peers, source, target, pair):
        copies = [
            pltpu.make_async_remote_copy(
                src_ref=source(peer), dst_ref=target.at[me], send_sem=sem.at[pair], recv_sem=sem.at[pair + 1],
                device_id={axis: peer},
            )
            for peer in peers
        ]
        for copy in copies:
            copy.start()

    def everything(axis, peers, target, pair):
        whole = target.at[pl.ds(0, len(peers))]
        return pltpu.make_async_remote_copy(
            src_ref=whole, dst_ref=whole, send_sem=sem.at[pair], recv_sem=sem.at[pair + 1], device_id={axis: peers[0]}
        )

    send("grp", g, group_peers, lambda peer: q_send, q_recv, 0)
    asking = everything("grp", group_peers, q_recv, 0)

    code = (table_v[pl.ds(0, 1), :] * 32 + table_v[pl.ds(1, 1), :]).astype(F32)
    counts = table_v[pl.ds(2, 1), :].astype(F32)
    mine = (g * 32).astype(F32)
    n_req = GROUPS * ROWS
    slot_row = mine + (iota((SLOTS * 8, n_req), 0) // 8).astype(F32)
    hit = slot_row == code
    slot_count = jnp.sum(jnp.where(hit, counts, 0.0), axis=1, keepdims=True)
    n_ask = GROUPS * QHEADS * ROWS
    table_row = iota((8, n_req), 0)
    both = jnp.where(table_row == 0, table_v[pl.ds(0, 1), :].astype(F32), table_v[pl.ds(1, 1), :].astype(F32))
    column = iota((n_req, n_ask), 1)
    spread = jnp.where(iota((n_req, n_ask), 0) == column // 32 * 8 + column % 8, 1.0, 0.0).astype(BF16)
    wide = matmul(both.astype(BF16), spread)
    wide_code = wide[0:1] * 32.0 + wide[1:2]
    ask_row = iota((SLOTS * 8, n_ask), 0)
    same_head = iota((SLOTS * 8, n_ask), 1) // 8 % 4 == ask_row % 8
    pick = jnp.where((mine + (ask_row // 8).astype(F32) == wide_code) & same_head, 1.0, 0.0).astype(BF16)
    code_col = jnp.sum(
        jnp.where(iota((n_req, n_req), 0) == iota((n_req, n_req), 1), code, 0.0), axis=1, keepdims=True
    )
    slot_lane = mine + (iota((n_req, 256), 1) // 8).astype(F32)
    hit_back = code_col == slot_lane
    r_lane = iota((n_req, 256), 1) % 8
    in_store = iota((n_req, 256), 1) < SLOTS * 8
    put_any = jnp.where(hit_back & in_store, 1.0, 0.0).astype(BF16)
    put = jnp.concatenate(
        [jnp.where(hit_back & in_store & (r_lane == i), 1.0, 0.0) for i in range(QHEADS)], axis=0
    ).astype(BF16)

    for step in range(SLOTS // IMG_STEP):
        arrived(ik_loads[step])
        for j in range(step * IMG_STEP, (step + 1) * IMG_STEP):
            ik_t[j] = ik_v[j].T

    k_acc = jnp.zeros((ROWS, KVW), F32)
    v_acc = jnp.zeros((ROWS, KVW), F32)
    for i in range(len(k_loads)):
        c = i * KV_CHUNK
        arrived(k_loads[i])
        k_acc = k_acc + matmul(normed[:, c : c + KV_CHUNK], kw_v[pl.ds(c, KV_CHUNK), :])
    for i in range(len(v_loads)):
        c = i * KV_CHUNK
        arrived(v_loads[i])
        v_acc = v_acc + matmul(normed[:, c : c + KV_CHUNK], vw_v[pl.ds(c, KV_CHUNK), :])
    new_keys = [head_norm(k_acc[:, i * HD : (i + 1) * HD], gains_v[pl.ds(1, 1), :]).astype(BF16).astype(F32) for i in range(2)]
    new_values = [v_acc[:, i * HD : (i + 1) * HD].astype(BF16).astype(F32) for i in range(2)]
    self_score = [jnp.sum(queries[i] * new_keys[i // 2], axis=-1, keepdims=True) for i in range(QHEADS)]

    for index in iv_loads:
        arrived(index)
    asking.wait_recv()
    asked = block_diagonal(matmul(pick, q_recv[...].reshape(n_ask, HD)))
    totals, tops, sums = [], [], []
    for first in range(0, SLOTS, IMG_GROUP):
        slots = range(first, first + IMG_GROUP)
        s = jnp.concatenate([matmul(asked[j * 8 : (j + 1) * 8], ik_t[j]) for j in slots], axis=0)
        valid = iota((IMG_GROUP * 8, IMG), 1).astype(F32) < slot_count[first * 8 : (first + IMG_GROUP) * 8]
        s = jnp.where(valid, s, NEG)
        top = jnp.max(s, axis=-1, keepdims=True)
        weights = jnp.where(valid, jnp.exp(s - top), 0.0).astype(BF16)
        tops.append(top)
        totals.append(jnp.sum(weights.astype(F32), axis=-1, keepdims=True))
        at = lambda j: (j - first) * 8
        sums += [own_half(matmul(weights[at(j) : at(j) + 8], iv_v[j])) for j in slots]
    total = jnp.concatenate(totals, axis=0)
    top = jnp.concatenate(tops, axis=0)
    some = total > 0.0
    safe = jnp.where(some, total, 1.0)
    mean_value = (jnp.concatenate(sums, axis=0) / safe).astype(BF16)
    level = jnp.where(some, top + jnp.log(safe), 0.0)
    high = level.astype(BF16).astype(F32)
    middle = (level - high).astype(BF16).astype(F32)
    low = level - high - middle
    part = iota((SLOTS * 8, HD), 1) % 32 // 8
    right_head = iota((SLOTS * 8, HD), 1) // 32 == iota((SLOTS * 8, HD), 0) % 8
    level_parts = jnp.where(part == 0, high, jnp.where(part == 1, middle, jnp.where(part == 2, low, 0.0)))
    level_parts = jnp.where(right_head, level_parts, 0.0).astype(BF16)
    pad = jnp.zeros((256 - SLOTS * 8, HD), BF16)
    values = jnp.concatenate([mean_value, pad], axis=0)
    back = [matmul(put[i * n_req : (i + 1) * n_req], values) for i in range(QHEADS)]
    back_levels = matmul(put_any, jnp.concatenate([level_parts, pad], axis=0))
    for p in range(GROUPS):
        here = slice(p * ROWS, (p + 1) * ROWS)
        slab = jnp.concatenate([b[here] for b in back] + [back_levels[here]], axis=0)
        back_send[p] = slab.astype(BF16)

    send("grp", g, group_peers, lambda peer: back_send.at[peer], back_recv, 2)
    answering = everything("grp", group_peers, back_recv, 2)
    back_recv[g] = back_send[g]

    for b in range(ROWS):
        if b % TEXT_STEP == 0:
            arrived(tk_loads[b // TEXT_STEP])
        q = block_diagonal(q_rows[pl.ds(b, 8, stride=8), :])
        s_text[pl.ds(b * 8, 8), :] = matmul_t(q, tk_v[b])
    place = iota((8, WINDOW), 1)
    for b in range(ROWS):
        if b % TEXT_STEP == 0:
            arrived(tv_loads[b // TEXT_STEP])
        p = jnp.sum(jnp.where(iota((8, ROWS), 1) == b, pos_v[...].astype(F32), 0.0), axis=1, keepdims=True)
        p = p.astype(jnp.int32)
        ok = (place < p) & (place != p % WINDOW)
        s = jnp.where(ok, s_text[pl.ds(b * 8, 8), :], NEG)
        top = jnp.max(s, axis=-1, keepdims=True)
        w = jnp.where(ok, jnp.exp(s - top), 0.0).astype(BF16)
        total = jnp.sum(w.astype(F32), axis=-1, keepdims=True)
        o_text[pl.ds(b * 8, 8), :] = own_half(matmul(w, tv_v[b]))
        m_text[pl.ds(b * 8, 8), :] = jnp.broadcast_to(top, (8, HD))
        l_text[pl.ds(b * 8, 8), :] = jnp.broadcast_to(total, (8, HD))

    rest = []
    for i in range(QHEADS):
        mt = m_text[pl.ds(i, ROWS, stride=8), :]
        lt = l_text[pl.ds(i, ROWS, stride=8), :]
        ot = o_text[pl.ds(i, ROWS, stride=8), :]
        own = jnp.broadcast_to(self_score[i], (ROWS, HD))
        top = jnp.maximum(mt, own)
        from_text = jnp.exp(mt - top)
        from_self = jnp.exp(own - top)
        rest.append((top, lt * from_text + from_self, ot * from_text + new_values[i // 2] * from_self))
    answering.wait_recv()
    image = back_recv[0].astype(F32)
    for p in range(1, GROUPS):
        image = image + back_recv[p].astype(F32)
    levels = image[QHEADS * ROWS : QHEADS * ROWS + ROWS]
    levels = levels + pltpu.roll(levels, HD - 8, 1) + pltpu.roll(levels, HD - 16, 1)
    attended = []
    for i in range(QHEADS):
        level = jnp.broadcast_to(levels[:, i * 32 : i * 32 + 1], (ROWS, HD))
        rest_top, rest_total, rest_sum = rest[i]
        top = jnp.maximum(level, rest_top)
        from_image = jnp.exp(level - top)
        from_rest = jnp.exp(rest_top - top)
        summed = image[i * ROWS : (i + 1) * ROWS] * from_image + rest_sum * from_rest
        attended.append(summed / (from_image + rest_total * from_rest))
    attended = jnp.concatenate(attended, axis=1).astype(BF16)

    for index in o_loads:
        arrived(index)
    half_width = D // 2
    pair_width = 1408
    pair_far = ring_x[2] // 2
    mate = 1 - 2 * (x_at - 2 * (x_at // 2))
    across = [ring_x[2], ring_x[2] + mate]
    for row, near in ((far_row, [x_at + mate, x_at]), (near_row, [x_at + mate])):
        for pair, peers in ((pair_far, across), (1 - pair_far, near)):
            start = row // 4 * half_width + pair * 1280
            part = matmul(attended, ow_v[:, pl.ds(pl.multiple_of(start, HD), pair_width)])
            for i in range(2):
                piece = part[:, i * 640 : i * 640 + WIDTH_PAD]
                low = pltpu.roll(piece, WIDTH_PAD - 32 * i, 1) if i else piece
                high = pltpu.roll(piece, WIDTH_PAD - 32 * i - 64, 1)
                rs_send[row + 2 * pair + i] = jnp.where(pair == 1, high, low).astype(SHARE)
            send("head", h, [row + x for x in peers], lambda peer: rs_send.at[peer], rs_recv, 4)
    sharing = everything("head", head_peers, rs_recv, 4)
    rs_recv[h] = rs_send[h]

    start = pl.multiple_of(h * WIDTH // 128 * 128, 128)
    aligned = hid_v[:, pl.ds(start, WIDTH_PAD)].astype(F32)
    residual = aligned
    for c in range(1, 4):
        residual = jnp.where(h % 4 == c, pltpu.roll(aligned, WIDTH_PAD - 32 * c, 1), residual)

    sharing.wait_recv()
    share = rs_recv[0].astype(F32)
    for p in range(1, HEADS):
        share = share + rs_recv[p].astype(F32)
    share = share[:, :WIDTH]
    own_squares = jnp.broadcast_to(jnp.sum(share * share, axis=-1, keepdims=True), (ROWS, 128))
    ss_send[...] = own_squares
    send("head", h, head_peers, lambda peer: ss_send, ss_recv, 6)
    squaring = everything("head", head_peers, ss_recv, 6)
    ss_recv[h] = own_squares
    squaring.wait_recv()
    squares = ss_recv[0]
    for p in range(1, HEADS):
        squares = squares + ss_recv[p]
    scale = lax.rsqrt(squares[:, :1] / D + EPS)
    out[...] = (residual[:, :WIDTH] + share * scale * post_v[...].reshape(1, WIDTH)).astype(BF16)

    for whole in (asking, answering, sharing, squaring):
        whole.wait_send()


def local(*args):
    (hidden, pre_gain, qw, kw, vw, ow, q_gain, k_gain, post_gain, tk, tv, pos, ik, iv, owner, slot, count) = args
    row = lambda v: v.reshape(1, -1)
    operands = [
        hidden, pre_gain.reshape(D // HD, HD), qw, kw, vw, ow, row(q_gain), row(k_gain), post_gain, tk, tv, row(pos), ik, iv,
        row(owner), row(slot), row(count),
    ]
    shapes = [pltpu.VMEM(v.shape, v.dtype) for v in operands[:14]]
    shapes[6:8] = [pltpu.VMEM((2, HD), F32)]
    shapes.append(pltpu.VMEM((3, HD), jnp.int32))
    dma = pltpu.SemaphoreType.DMA
    n_loads = len(Q_CHUNKS) + 2 * (D // KV_CHUNK) + D // OW_CHUNK + 2 * (SLOTS // IMG_STEP) + 2 * (ROWS // TEXT_STEP)
    scratch = shapes + [
        pltpu.VMEM((64, HD), F32),
        pltpu.VMEM((QHEADS * ROWS, HD), BF16),
        pltpu.VMEM((GROUPS, QHEADS * ROWS, HD), BF16),
        pltpu.VMEM((ROWS * 8, WINDOW), F32),
        pltpu.VMEM((ROWS * 8, HD), F32),
        pltpu.VMEM((ROWS * 8, HD), F32),
        pltpu.VMEM((ROWS * 8, HD), F32),
        pltpu.VMEM((SLOTS, KVW, IMG), BF16),
        pltpu.VMEM((GROUPS, 40, HD), BF16),
        pltpu.VMEM((GROUPS, 40, HD), BF16),
        pltpu.VMEM((HEADS, ROWS, WIDTH_PAD), SHARE),
        pltpu.VMEM((HEADS, ROWS, WIDTH_PAD), SHARE),
        pltpu.VMEM((ROWS, 128), F32),
        pltpu.VMEM((HEADS, ROWS, 128), F32),
        dma((6,)),
        dma((n_loads,)),
        dma((8,)),
    ]
    return pl.pallas_call(
        layer_kernel,
        out_shape=pltpu.VMEM((ROWS, WIDTH), BF16),
        in_specs=[pl.BlockSpec(memory_space=pl.ANY)] * len(operands),
        out_specs=pl.BlockSpec(memory_space=pltpu.VMEM),
        scratch_shapes=scratch,
        compiler_params=pltpu.CompilerParams(
            collective_id=0, has_side_effects=True, vmem_limit_bytes=60 * 1024 * 1024
        ),
    )(*operands)


def solution(mesh):
    placed = (
        P("grp", None),
        P(),
        P(None, "head"),
        P(None, "head"),
        P(None, "head"),
        P("head", None),
        P(),
        P(),
        P("head"),
        P("grp", None, "head"),
        P("grp", None, "head"),
        P("grp"),
        P("grp", None, "head"),
        P("grp", None, "head"),
        P(),
        P(),
        P(),
    )
    return jax.shard_map(
        local, mesh=mesh, in_specs=placed, out_specs=P("grp", "head"), check_vma=False
    )
```
